256 devices in a mesh: groups: 2 (over z), ep: 64 (over y, x), tp: 2 (over core).
Axes of the slice: x: 8, y: 8, z: 2, core: 2. Of those that a mesh axis runs over, the one named last changes fastest.
The devices are a block of a 8x8x16 slice.
Arguments:
- hidden: bfloat16 [2048, 3584], P(('groups', 'ep'), 'tp'), parts along dimension 0, may hold values from -6 to 6
- routes: int32 [2048, 8], P(('groups', 'ep')), parts along dimension 0, may hold values from 0 to 63, as said below
- router_weight: bfloat16 [3584, 64], P('tp'), may hold values from -0.1875 to 0.1875
- gate_weight: bfloat16 [64, 3584, 1024], P('ep', None, 'tp'), may hold values from -0.09375 to 0.09375
- up_weight: bfloat16 [64, 3584, 1024], P('ep', None, 'tp'), may hold values from -0.09375 to 0.09375
- down_weight: bfloat16 [64, 1024, 3584], P('ep', 'tp'), may hold values from -0.1875 to 0.1875
- q_latent: bfloat16 [512, 64, 512], P(('groups', 'ep'), 'tp'), parts along dimension 0, may hold values from -48 to 48
- q_rope: bfloat16 [512, 64, 64], P(('groups', 'ep'), 'tp'), parts along dimension 0, may hold values from -48 to 48
- cache_latent: bfloat16 [512, 256, 512], P(('groups', 'ep')), parts along dimension 0, may hold values from -4 to 4
- cache_rope: bfloat16 [512, 64, 256], P(('groups', 'ep')), parts along dimension 0, may hold values from -4 to 4
- lengths: int32 [512], P(('groups', 'ep')), parts along dimension 0, may hold values from 16 to 256, as said below
Outputs:
- moe_out: bfloat16 [2048, 3584], P(('groups', 'ep'), 'tp'), parts along dimension 0
- attn_latent: bfloat16 [512, 64, 512], P(('groups', 'ep'), 'tp'), parts along dimension 0
The draws below stay inside these ranges and needn't reach their ends.
There are 2 independent parts, one for each index of `groups`. The reference program is written for one: setup_inputs(seed, part) draws one part's arguments, and reference() takes and returns one part's arrays. A program takes and returns all parts, laid end to end along the dimension named above; an argument that names none is the same for every part. Nothing has to cross between parts.
Inputs may be any that keep to these rules, and one draw needn't show every extreme that they name: `routes`: each row names 8 different experts; in each aligned block of 16 rows (the rows of one index of ep) no expert is named more than 8 times, and one expert, the same in every block, is named exactly 8 times in each block. `lengths`: one sequence has 256 live positions and one has 16.
All inputs are finite; a program needn't handle non-finite values.
Results may differ from the reference program's by a relative error of at most 0.0085.
Values may be sent and summed in bfloat16 or wider, within the bound.
No kernel may reach another device: no remote copies, remote signals or barrier semaphores. Data moves between devices by JAX's collectives and lax.ppermute only.
A program may use at most 128 MiB of HBM per device.

```python
import jax
import jax.numpy as jnp
from jax import lax

D = 3584
FFW = 1024
LAT = 512
ROPE = 64
HEADS = 64
TOK_DEV = 16
CACHE = 256
EXPERTS = 64
TOP = 8
CAP = 8
TOKENS = 1024
SEQS = 256


def cache_parts(key):
    latent_key, rope_key = jax.random.split(jax.random.fold_in(key, 7))
    latent = jnp.clip(jax.random.normal(latent_key, (SEQS, CACHE, LAT), jnp.float32), -4.0, 4.0)
    rotary = jnp.clip(jax.random.normal(rope_key, (SEQS, ROPE, CACHE), jnp.float32), -4.0, 4.0)
    return (latent.astype(jnp.bfloat16).astype(jnp.float32), rotary.astype(jnp.bfloat16).astype(jnp.float32))


def query_parts(key):
    query_key = jax.random.fold_in(key, 13)
    keys = jax.random.split(query_key, 1)
    query_bound = 48.0 * 576.0 / (LAT + ROPE)
    queries = jnp.clip(1.15 * jax.random.normal(keys[0], (SEQS, HEADS, LAT + ROPE), jnp.float32), -5.0, 5.0)
    queries = jnp.clip(queries, -query_bound, query_bound)
    return (queries[:, :, :LAT], queries[:, :, LAT:])


def draw_q_latent(key, part):
    return query_parts(key)[0].astype(jnp.bfloat16)


def draw_q_rope(key, part):
    return query_parts(key)[1].astype(jnp.bfloat16)


def draw_cache_latent(key, part):
    return cache_parts(key)[0].astype(jnp.bfloat16)


def draw_cache_rope(key, part):
    return cache_parts(key)[1].astype(jnp.bfloat16)


def draw_lengths(key, part):
    keys = jax.random.split(jax.random.fold_in(key, 3), 3)
    shortest_len = CACHE // 16
    drawn_lengths = jax.random.randint(keys[0], (SEQS,), shortest_len, CACHE + 1, dtype=jnp.int32)
    longest_at = jax.random.randint(keys[1], (), 0, SEQS, dtype=jnp.int32)
    shortest_at = (longest_at + 1 + jax.random.randint(keys[2], (), 0, SEQS - 1, dtype=jnp.int32)) % SEQS
    drawn_lengths = drawn_lengths.at[longest_at].set(CACHE).at[shortest_at].set(shortest_len)
    return drawn_lengths.astype(jnp.int32)


def draw_routes(key, part):
    block_count = TOKENS // TOK_DEV
    others = EXPERTS - 1
    remaining = TOK_DEV * TOP - CAP
    base_load = remaining // others
    extra_count = remaining % others
    pair_count = others // 2
    reach = min(base_load, CAP - base_load - 1)
    keys = jax.random.split(jax.random.fold_in(key, 5), 3)
    expert_order = jax.random.permutation(keys[0], EXPERTS).astype(jnp.int32)
    shifts = jax.random.randint(keys[1], (block_count, pair_count), 0, reach + 1, dtype=jnp.int32)
    other_loads = base_load + (jnp.arange(others, dtype=jnp.int32) < extra_count).astype(jnp.int32)
    other_loads = jnp.broadcast_to(other_loads[None, :], (block_count, others))
    other_loads = other_loads.at[:, 0:2 * pair_count:2].add(-shifts)
    other_loads = other_loads.at[:, 1:2 * pair_count:2].add(shifts)
    loads = jnp.concatenate([jnp.full((block_count, 1), CAP, jnp.int32), other_loads], axis=1)
    ends = jnp.cumsum(loads, axis=1).astype(jnp.int32)
    position = jnp.arange(TOK_DEV * TOP, dtype=jnp.int32)
    which = jnp.sum((position[None, :, None] >= ends[:, None, :]).astype(jnp.int32), axis=2)
    listed = expert_order[which]
    table = jnp.transpose(listed.reshape(block_count, TOP, TOK_DEV), (0, 2, 1))
    token_perms = jax.vmap(lambda sub_key: jax.random.permutation(sub_key, TOK_DEV))(jax.random.split(keys[2], block_count))
    table = jax.vmap(lambda rows_table, perm_order: rows_table[perm_order])(table, token_perms)
    return table.reshape(TOKENS, TOP).astype(jnp.int32)


def levels(key, shape, cuts, low, top_value):
    def one(axis_at, shards_of):
        steps = jax.random.uniform(jax.random.fold_in(jax.random.fold_in(key, 6), axis_at), (shards_of,), jnp.float32, low / len(cuts), top_value / len(cuts))
        return jnp.repeat(jnp.exp(steps), shape[axis_at] // shards_of).reshape((-1,) + (1,) * (len(shape) - axis_at - 1))

    gain = one(*cuts[0])
    for cut in cuts[1:]:
        gain = gain * one(*cut)
    return gain


def normal_values(key, extent, scale, bound, cuts=(), kind=jnp.bfloat16):
    entries = jax.random.normal(key, extent, jnp.float32) * scale
    if len(cuts) > 0:
        entries = levels(key, extent, cuts, -0.22, 0.18) * entries
    return jnp.clip(entries, min=-bound, max=bound).astype(kind)


def setup_inputs(seed: int = 0, part: int = 0) -> dict:
    streams_of = jax.random.split(jax.random.key(seed), 12)
    own_keys = jax.random.split(jax.random.fold_in(streams_of[11], part), 12)
    return {
        "hidden": normal_values(own_keys[0], (TOKENS, D), 1.0, 6.0, ((0, 64), (1, 2))),
        "routes": draw_routes(jax.random.fold_in(jax.random.fold_in(streams_of[11], part), 71), part),
        "router_weight": normal_values(streams_of[2], (D, EXPERTS), (D // 4) ** -0.5, 0.1875, ((0, 2),)),
        "gate_weight": normal_values(streams_of[3], (EXPERTS, D, FFW), D ** -0.5, 0.09375, ((0, 64), (2, 2))),
        "up_weight": normal_values(streams_of[4], (EXPERTS, D, FFW), D ** -0.5, 0.09375, ((0, 64), (2, 2))),
        "down_weight": normal_values(streams_of[5], (EXPERTS, FFW, D), FFW ** -0.5, 0.1875, ((0, 64), (1, 2))),
        "q_latent": draw_q_latent(jax.random.fold_in(jax.random.fold_in(streams_of[11], part), 71), part),
        "q_rope": draw_q_rope(jax.random.fold_in(jax.random.fold_in(streams_of[11], part), 71), part),
        "cache_latent": draw_cache_latent(jax.random.fold_in(jax.random.fold_in(streams_of[11], part), 71), part),
        "cache_rope": draw_cache_rope(jax.random.fold_in(jax.random.fold_in(streams_of[11], part), 71), part),
        "lengths": draw_lengths(jax.random.fold_in(jax.random.fold_in(streams_of[11], part), 71), part),
    }


softmax_scale = 192.0 ** -0.5
routed_scale = 2.5
block_rows = 32


def expert_block(hidden, gate_weight, up_weight, down_weight, token_index, expert_index):
    picked = jnp.take(hidden, token_index, axis=0)
    gate_part = jnp.dot(picked, gate_weight[expert_index], preferred_element_type=jnp.float32)
    up_part = jnp.dot(picked, up_weight[expert_index], preferred_element_type=jnp.float32)
    active = (jax.nn.silu(gate_part) * up_part).astype(jnp.bfloat16)
    return jnp.dot(active, down_weight[expert_index], preferred_element_type=jnp.float32).astype(jnp.bfloat16)


def routed_rows(hidden, routes, gate_weight, up_weight, down_weight):
    total = TOKENS * TOP
    block_count = (total + block_rows - 1) // block_rows + EXPERTS
    flat_ids = routes.reshape(-1).astype(jnp.int32)
    order = jnp.argsort(flat_ids, stable=True).astype(jnp.int32)
    counts = jnp.zeros((EXPERTS,), jnp.int32).at[flat_ids].add(1)
    padded = ((counts + block_rows - 1) // block_rows * block_rows).astype(jnp.int32)
    padded_end = jnp.cumsum(padded).astype(jnp.int32)
    padded_start = (padded_end - padded).astype(jnp.int32)
    seg_start = (jnp.cumsum(counts) - counts).astype(jnp.int32)
    sorted_ids = flat_ids[order]
    within = jnp.arange(total, dtype=jnp.int32) - seg_start[sorted_ids]
    target = (padded_start[sorted_ids] + within).astype(jnp.int32)
    token_of = jnp.zeros((block_count * block_rows,), jnp.int32).at[target].set((order // TOP).astype(jnp.int32))
    block_start = jnp.arange(block_count, dtype=jnp.int32) * block_rows
    block_expert = jnp.sum((block_start[:, None] >= padded_end[None, :]).astype(jnp.int32), axis=1).astype(jnp.int32)
    block_expert = jnp.minimum(block_expert, EXPERTS - 1).astype(jnp.int32)

    def one_block(item):
        token_index, expert_index = item
        return expert_block(hidden, gate_weight, up_weight, down_weight, token_index, expert_index)

    outputs = lax.map(one_block, (token_of.reshape(block_count, block_rows), block_expert))
    outputs = outputs.reshape(block_count * block_rows, D)
    slot_of = jnp.zeros((total,), jnp.int32).at[order].set(target)
    return jnp.take(outputs, slot_of, axis=0).reshape(TOKENS, TOP, D)


def attention(q_latent, q_rope, cache_latent, cache_rope, lengths):
    scores = jnp.einsum("bhl,bjl->bhj", q_latent.astype(jnp.float32), cache_latent.astype(jnp.float32))
    scores = scores + jnp.einsum("bhr,brj->bhj", q_rope.astype(jnp.float32), cache_rope.astype(jnp.float32))
    scores = scores * softmax_scale
    position = jnp.arange(CACHE, dtype=jnp.int32)
    live = position[None, None, :] < lengths.astype(jnp.int32)[:, None, None]
    scores = jnp.where(live, scores, -jnp.inf)
    highest = jnp.max(scores, axis=2, keepdims=True)
    expo = jnp.where(live, jnp.exp(scores - highest), 0.0)
    probs = (expo / jnp.sum(expo, axis=2, keepdims=True)).astype(jnp.bfloat16)
    mixed = jnp.einsum("bhj,bjl->bhl", probs.astype(jnp.float32), cache_latent.astype(jnp.float32))
    return mixed.astype(jnp.bfloat16)


def reference(hidden, routes, router_weight, gate_weight, up_weight, down_weight, q_latent, q_rope, cache_latent, cache_rope, lengths):
    logits = jnp.dot(hidden, router_weight, preferred_element_type=jnp.float32)
    affinity = jax.nn.sigmoid(logits)
    chosen = jnp.take_along_axis(affinity, routes.astype(jnp.int32), axis=1)
    gates = routed_scale * chosen / jnp.sum(chosen, axis=1, keepdims=True)
    expert_out = routed_rows(hidden, routes, gate_weight, up_weight, down_weight)
    moe_out = jnp.sum(gates[:, :, None] * expert_out.astype(jnp.float32), axis=1).astype(jnp.bfloat16)
    attn_latent = attention(q_latent, q_rope, cache_latent, cache_rope, lengths)
    return (moe_out, attn_latent)
```

```python
import jax
import jax.numpy as jnp
from jax import lax
from jax.sharding import PartitionSpec as P

softmax_scale = 192.0 ** (-0.5)
routed_scale = 2.5


def gathered_total(value, axis):
    tiles = lax.all_gather(value, axis)
    return tiles.sum(axis=0)


def swapped(value, axis):
    return lax.ppermute(value, axis, [(0, 1), (1, 0)])


def half_dot(rows, weight, start):
    part = lax.dynamic_slice_in_dim(weight, start, rows.shape[1], 0)
    return jnp.dot(rows, part, preferred_element_type=jnp.float32)


def half_out(rows, weight, start, width):
    part = lax.dynamic_slice_in_dim(weight, start, width, 1)
    return jnp.dot(rows, part, preferred_element_type=jnp.float32)


def local(
    hidden,
    routes,
    router_weight,
    gate_weight,
    up_weight,
    down_weight,
    q_latent,
    q_rope,
    cache_latent,
    cache_rope,
    lengths,
):
    token_count, top_count = routes.shape
    expert_count = lax.axis_size("ep")
    capacity = min(token_count, 4 * token_count * top_count // expert_count)
    partial_logits = jnp.dot(hidden, router_weight, preferred_element_type=jnp.float32)
    logits = gathered_total(partial_logits, "tp")
    affinity = jax.nn.sigmoid(logits)
    expert_iota = jnp.arange(expert_count, dtype=jnp.int32)
    chosen_mask = routes[:, :, None] == expert_iota[None, None, :]
    chosen = jnp.sum(jnp.where(chosen_mask, affinity[:, None, :], 0.0), axis=2)
    gates = routed_scale * chosen / jnp.sum(chosen, axis=1, keepdims=True)
    flat_mask = chosen_mask.reshape(token_count * top_count, expert_count).astype(jnp.int32)
    earlier = jnp.cumsum(flat_mask, axis=0) - flat_mask
    within = jnp.sum(flat_mask * earlier, axis=1).reshape(token_count, top_count)
    slot_index = routes * capacity + within
    slot_iota = jnp.arange(expert_count * capacity, dtype=jnp.int32)
    placing = jnp.sum(
        (slot_index[None, :, :] == slot_iota[:, None, None]).astype(jnp.int32), axis=2
    )
    placing = placing.astype(jnp.bfloat16)
    outgoing = jnp.dot(placing, hidden, preferred_element_type=jnp.float32).astype(jnp.bfloat16)
    outgoing = outgoing.reshape(expert_count, capacity, hidden.shape[1])
    received = lax.all_to_all(outgoing, "ep", split_axis=0, concat_axis=0, tiled=True)
    source_count, slot_count, half = received.shape
    own_rows = received.reshape(source_count * slot_count, half)
    other_rows = swapped(own_rows, "tp")
    mine = lax.axis_index("tp") * half
    theirs = half - mine
    gate_part = half_dot(own_rows, gate_weight[0], mine) + half_dot(other_rows, gate_weight[0], theirs)
    up_part = half_dot(own_rows, up_weight[0], mine) + half_dot(other_rows, up_weight[0], theirs)
    active = (jax.nn.silu(gate_part) * up_part).astype(jnp.bfloat16)
    sent_part = half_out(active, down_weight[0], theirs, half).astype(jnp.bfloat16)
    kept_part = half_out(active, down_weight[0], mine, half)
    summed = (kept_part + swapped(sent_part, "tp").astype(jnp.float32)).astype(jnp.bfloat16)
    summed = summed.reshape(source_count, slot_count, half)
    returned = lax.all_to_all(summed, "ep", split_axis=0, concat_axis=0, tiled=True)
    scores = jnp.einsum("bhl,bjl->bhj", q_latent, cache_latent, preferred_element_type=jnp.float32)
    scores = scores + jnp.einsum(
        "bhr,brj->bhj", q_rope, cache_rope, preferred_element_type=jnp.float32
    )
    scores = scores * softmax_scale
    position = jnp.arange(cache_latent.shape[1], dtype=jnp.int32)
    live = position[None, None, :] < lengths[:, None, None]
    scores = jnp.where(live, scores, -jnp.inf)
    highest = jnp.max(scores, axis=2, keepdims=True)
    expo = jnp.where(live, jnp.exp(scores - highest), 0.0)
    attn_probs = (expo / jnp.sum(expo, axis=2, keepdims=True)).astype(jnp.bfloat16)
    attn_latent = jnp.einsum(
        "bhj,bjl->bhl", attn_probs, cache_latent, preferred_element_type=jnp.float32
    )
    attn_latent = attn_latent.astype(jnp.bfloat16)
    returned_flat = returned.reshape(expert_count * capacity, returned.shape[2])
    picked = jnp.take(returned_flat, slot_index.reshape(-1), axis=0).reshape(
        token_count, top_count, returned.shape[2]
    )
    moe_out = jnp.sum(gates[:, :, None] * picked.astype(jnp.float32), axis=1).astype(jnp.bfloat16)
    return (moe_out, attn_latent)


def solution(mesh):
    return jax.shard_map(
        local,
        mesh=mesh,
        in_specs=(
            P(("groups", "ep"), "tp"),
            P(("groups", "ep"), None),
            P("tp", None),
            P("ep", None, "tp"),
            P("ep", None, "tp"),
            P("ep", "tp", None),
            P(("groups", "ep"), "tp", None),
            P(("groups", "ep"), "tp", None),
            P(("groups", "ep"), None, None),
            P(("groups", "ep"), None, None),
            P(("groups", "ep")),
        ),
        out_specs=(P(("groups", "ep"), "tp"), P(("groups", "ep"), "tp", None)),
        check_vma=False,
    )
```

```python
import math

import jax
import jax.numpy as jnp
from jax import lax
from jax.sharding import PartitionSpec as P

softmax_scale = 192.0 ** (-0.5)
routed_scale = 2.5
pair = ("ep", "tp")


def side_of(devices):
    side = math.isqrt(devices)
    assert side * side == devices
    return side


def flat_index(first, second, core, side):
    row, column = (second, first) if core == 0 else (first, second)
    return (row * side + column) * 2 + core


def first_groups(side):
    return [
        [flat_index(first, second, core, side) for first in range(side)]
        for core in range(2)
        for second in range(side)
    ]


def shifted(value, shift, side):
    moves = []
    for core in range(2):
        for first in range(side):
            for second in range(side):
                target = (second + shift) % side
                moves.append(
                    (flat_index(first, second, core, side), flat_index(first, target, core, side))
                )
    return lax.ppermute(value, pair, moves)


def swapped(value, axis):
    return lax.ppermute(value, axis, [(0, 1), (1, 0)])


def half_dot(rows, weight, start):
    part = lax.dynamic_slice_in_dim(weight, start, rows.shape[1], 0)
    return jnp.dot(rows, part, preferred_element_type=jnp.float32)


def half_out(rows, weight, start, width):
    part = lax.dynamic_slice_in_dim(weight, start, width, 1)
    return jnp.dot(rows, part, preferred_element_type=jnp.float32)


def split_in_two(value):
    high = value.astype(jnp.bfloat16)
    return high, (value - high.astype(jnp.float32)).astype(jnp.bfloat16)


def attention(q_latent, q_rope, cache_latent, cache_rope, lengths):
    scores = jnp.einsum("bhl,bjl->bhj", q_latent, cache_latent, preferred_element_type=jnp.float32)
    scores = scores + jnp.einsum(
        "bhr,brj->bhj", q_rope, cache_rope, preferred_element_type=jnp.float32
    )
    scores = scores * softmax_scale
    position = jnp.arange(cache_latent.shape[1], dtype=jnp.int32)
    live = position[None, None, :] < lengths[:, None, None]
    scores = jnp.where(live, scores, -jnp.inf)
    highest = jnp.max(scores, axis=2, keepdims=True)
    expo = jnp.where(live, jnp.exp(scores - highest), 0.0)
    attn_probs = (expo / jnp.sum(expo, axis=2, keepdims=True)).astype(jnp.bfloat16)
    attn_latent = jnp.einsum(
        "bhj,bjl->bhl", attn_probs, cache_latent, preferred_element_type=jnp.float32
    )
    return attn_latent.astype(jnp.bfloat16)


def local(
    hidden,
    routes,
    router_weight,
    gate_weight,
    up_weight,
    down_weight,
    q_latent,
    q_rope,
    cache_latent,
    cache_rope,
    lengths,
):
    token_count, top_count = routes.shape
    expert_count = lax.axis_size("ep")
    side = side_of(expert_count)
    capacity = min(token_count, 4 * token_count * top_count // expert_count)
    line_slots = side * capacity
    line_tokens = side * token_count
    half = hidden.shape[1]
    bf16, f32 = jnp.bfloat16, jnp.float32

    core = lax.axis_index("tp")
    place = lax.axis_index("ep")
    row, column = place // side, place % side
    first = jnp.where(core == 0, column, row)
    second = jnp.where(core == 0, row, column)
    side_iota = jnp.arange(side, dtype=jnp.int32)

    expert_iota = jnp.arange(expert_count, dtype=jnp.int32)
    mask = jnp.sum((routes.T[:, :, None] == expert_iota).astype(f32), axis=0)
    partial_logits = jnp.dot(hidden, router_weight, preferred_element_type=f32)
    logits = partial_logits + swapped(partial_logits, "tp")
    chosen = jnp.where(mask > 0, jax.nn.sigmoid(logits), 0.0)
    gates = routed_scale * chosen / jnp.sum(chosen, axis=1, keepdims=True)

    ahead = (second + side_iota) % side
    experts = jnp.where(
        core == 0, ahead[None, :] * side + side_iota[:, None], side_iota[:, None] * side + ahead[None, :]
    )
    lanes = 128 * ((2 * side + 127) // 128)
    blank = jnp.full((side, lanes - 2 * side), -1, jnp.int32)
    wanted = jnp.concatenate([experts, expert_count + experts, blank], axis=1)
    source = jnp.arange(2 * expert_count, dtype=jnp.int32)
    gate_select = (wanted[:, None, :] == source[None, :, None]).astype(bf16)
    gate_parts = jnp.concatenate(split_in_two(gates), axis=1)
    gate_lanes = jnp.einsum("te,pec->ptc", gate_parts, gate_select, preferred_element_type=f32)
    message = jnp.concatenate(
        [jnp.broadcast_to(hidden[None], (side, token_count, half)), gate_lanes.astype(bf16)], axis=2
    )
    line = lax.all_to_all(
        message, pair, 0, 0, axis_index_groups=first_groups(side), tiled=True
    )
    tokens = line[:, :, :half].reshape(line_tokens, half)
    line_gates = line[:, :, half : half + 2 * side].reshape(line_tokens, 2 * side).T
    gate_high, gate_low = line_gates[:side], line_gates[side:]

    picked = gate_high != 0
    token_iota = jnp.arange(line_tokens, dtype=jnp.int32)
    block_of = token_iota // token_count
    before = (token_iota[:, None] < token_iota[None, :]) & (block_of[:, None] == block_of[None, :])
    rank = jnp.dot(picked.astype(bf16), before.astype(bf16), preferred_element_type=f32)
    offset = ((first - block_of + side) % side) * capacity
    slot = jnp.where(picked, offset[None, :] + rank.astype(jnp.int32), -1)
    slot_iota = jnp.arange(line_slots, dtype=jnp.int32)
    placed = slot[:, None, :] == slot_iota[None, :, None]
    placing = placed.astype(bf16).reshape(side * line_slots, line_tokens)
    rows = jnp.dot(placing, tokens, preferred_element_type=f32).astype(bf16)
    rows = rows.reshape(side, line_slots, half)

    own = [rows[0]] + [shifted(rows[step], step, side) for step in range(1, side)]
    blocks = [part.reshape(side, capacity, half) for part in own]
    own_rows = jnp.concatenate(own, axis=0)
    turned = jnp.stack(blocks, axis=1).reshape(side * line_slots, half)
    other_rows = swapped(turned, "tp")

    attn_latent = attention(q_latent, q_rope, cache_latent, cache_rope, lengths)

    mine = core * half
    theirs = half - mine
    gate_part = half_dot(own_rows, gate_weight[0], mine) + half_dot(other_rows, gate_weight[0], theirs)
    up_part = half_dot(own_rows, up_weight[0], mine) + half_dot(other_rows, up_weight[0], theirs)
    active = (jax.nn.silu(gate_part) * up_part).astype(bf16)
    sent = half_out(active, down_weight[0], theirs, half).astype(bf16)
    sent = jnp.swapaxes(sent.reshape(side, side, capacity, half), 0, 1)
    kept = half_out(active, down_weight[0], mine, half)
    arrived = swapped(sent.reshape(side * line_slots, half), "tp")
    summed = (kept + arrived.astype(f32)).astype(bf16).reshape(side, line_slots, half)

    back = [summed[0]] + [shifted(summed[step], -step, side) for step in range(1, side)]
    back = jnp.concatenate(back, axis=0)
    taking = jnp.concatenate(
        [
            jnp.where(placed, part[:, None, :], 0).reshape(side * line_slots, line_tokens)
            for part in (gate_high, gate_low)
        ],
        axis=1,
    )
    weighted = lax.dot_general(
        taking, back, (((0,), (0,)), ((), ())), preferred_element_type=f32
    )
    weighted = (weighted[:line_tokens] + weighted[line_tokens:]).astype(bf16)
    weighted = weighted.reshape(side, token_count, half)
    shares = lax.all_to_all(
        weighted, pair, 0, 0, axis_index_groups=first_groups(side), tiled=True
    )
    moe_out = jnp.sum(shares.astype(f32), axis=0).astype(bf16)
    return (moe_out, attn_latent)


def solution(mesh):
    return jax.shard_map(
        local,
        mesh=mesh,
        in_specs=(
            P(("groups", "ep"), "tp"),
            P(("groups", "ep"), None),
            P("tp", None),
            P("ep", None, "tp"),
            P("ep", None, "tp"),
            P("ep", "tp", None),
            P(("groups", "ep"), "tp", None),
            P(("groups", "ep"), "tp", None),
            P(("groups", "ep"), None, None),
            P(("groups", "ep"), None, None),
            P(("groups", "ep")),
        ),
        out_specs=(P(("groups", "ep"), "tp"), P(("groups", "ep"), "tp", None)),
        check_vma=False,
    )
```

```python
import math

import jax
import jax.numpy as jnp
from jax import lax
from jax.experimental import pallas as pl
from jax.experimental.pallas import tpu as pltpu
from jax.sharding import PartitionSpec as P

softmax_scale = 192.0 ** (-0.5)
routed_scale = 2.5
pair = ("ep", "tp")


def side_of(devices):
    side = math.isqrt(devices)
    assert side * side == devices
    return side


def flat_index(first, second, core, side):
    row, column = (second, first) if core == 0 else (first, second)
    return (row * side + column) * 2 + core


def first_groups(side):
    return [
        [flat_index(first, second, core, side) for first in range(side)]
        for core in range(2)
        for second in range(side)
    ]


def shifted(value, shift, side):
    moves = []
    for core in range(2):
        for first in range(side):
            for second in range(side):
                target = (second + shift) % side
                moves.append(
                    (flat_index(first, second, core, side), flat_index(first, target, core, side))
                )
    return lax.ppermute(value, pair, moves)


def swapped(value, axis):
    return lax.ppermute(value, axis, [(0, 1), (1, 0)])


def on_chip(kernel, out_shapes, operands, name, scratch=(), limit=16):
    return pl.pallas_call(
        kernel,
        out_shape=out_shapes,
        in_specs=[
            pl.BlockSpec(memory_space=pltpu.SMEM if a.ndim == 1 else pltpu.VMEM) for a in operands
        ],
        out_specs=jax.tree.map(lambda _: pl.BlockSpec(memory_space=pltpu.VMEM), out_shapes),
        scratch_shapes=list(scratch),
        compiler_params=pltpu.CompilerParams(vmem_limit_bytes=limit * 1024 * 1024),
        name=name,
    )(*operands)


def fetch_kernel(*refs):
    count = (len(refs) - 1) // 3
    sources, targets, sems = refs[:count], refs[count + 1 : 2 * count + 1], refs[2 * count + 1 :]
    copies = [pltpu.make_async_copy(s, t, m) for s, t, m in zip(sources, targets, sems)]
    for copy in copies:
        copy.start()
    for copy in copies:
        copy.wait()


def fetched(arrays, after):
    return pl.pallas_call(
        fetch_kernel,
        out_shape=tuple(pltpu.VMEM(a.shape, a.dtype) for a in arrays),
        in_specs=[pl.BlockSpec(memory_space=pltpu.HBM)] * len(arrays)
        + [pl.BlockSpec(memory_space=pl.ANY)],
        out_specs=tuple([pl.BlockSpec(memory_space=pltpu.VMEM)] * len(arrays)),
        scratch_shapes=[pltpu.SemaphoreType.DMA] * len(arrays),
        compiler_params=pltpu.CompilerParams(vmem_limit_bytes=42 * 1024 * 1024),
        name="fetch_weights",
    )(*arrays, after)


def select_kernel(slot_ref, line_ref, *part_refs):
    side, line_tokens = slot_ref.shape
    slots, half = part_refs[0].shape
    tokens = line_ref[:, :, :half].reshape(line_tokens, half)
    slot_iota = lax.broadcasted_iota(jnp.int32, (slots, line_tokens), 0)
    for step in range(side):
        placing = (slot_ref[step : step + 1, :] == slot_iota).astype(jnp.float32).astype(jnp.bfloat16)
        rows = jnp.dot(placing, tokens, preferred_element_type=jnp.float32)
        part_refs[step][...] = rows.astype(jnp.bfloat16)


def near_to_far(side):
    return sorted(range(side), key=lambda step: (min(step, side - step), step))


def by_step(parts):
    steps = near_to_far(len(parts))
    return [parts[steps.index(step)] for step in range(len(parts))]


def expert_kernel(side, start_ref, gate_ref, up_ref, down_ref, *refs):
    own_refs, other_refs = by_step(refs[:side]), by_step(refs[side : 2 * side])
    active_ref, sent_ref, own, other = refs[2 * side :]
    slots, half = own_refs[0].shape
    capacity = slots // side
    width = gate_ref.shape[1]
    for step in range(side):
        rows = pl.ds(step * slots, slots)
        own[rows, :] = own_refs[step][...]
        for block in range(side):
            other[pl.ds(step * slots + block * capacity, capacity), :] = other_refs[block][
                pl.ds(step * capacity, capacity), :
            ]
    mine = pl.multiple_of(start_ref[0], 256)
    theirs = pl.multiple_of(half - mine, 256)

    def product(weight_ref, columns):
        return jnp.dot(
            own[...], weight_ref[pl.ds(mine, half), columns], preferred_element_type=jnp.float32
        ) + jnp.dot(
            other[...], weight_ref[pl.ds(theirs, half), columns], preferred_element_type=jnp.float32
        )

    tile = 256
    for column in range(0, width, tile):
        columns = pl.ds(column, tile)
        gate_part = product(gate_ref, columns)
        up_part = product(up_ref, columns)
        active_ref[:, columns] = (jax.nn.silu(gate_part) * up_part).astype(jnp.bfloat16)
    active = active_ref[...]
    for column in range(0, half, tile):
        weight = down_ref[:, pl.ds(pl.multiple_of(theirs + column, 256), tile)]
        sent = jnp.dot(active, weight, preferred_element_type=jnp.float32).astype(jnp.bfloat16)
        sent = sent.reshape(side, side, capacity, tile)
        for block in range(side):
            sent_ref[block, :, :, pl.ds(column, tile)] = sent[:, block]


def finish_kernel(start_ref, active_ref, down_ref, arrived_ref, *part_refs):
    side = len(part_refs)
    slots, half = part_refs[0].shape
    mine = start_ref[0]
    tile = 256
    for column in range(0, half, tile):
        columns = pl.ds(column, tile)
        weight = down_ref[:, pl.ds(pl.multiple_of(mine + column, 256), tile)]
        kept = jnp.dot(active_ref[...], weight, preferred_element_type=jnp.float32)
        for step in range(side):
            rows = pl.ds(step * slots, slots)
            arrived = arrived_ref[rows, columns].astype(jnp.float32)
            part_refs[step][:, columns] = (
                kept[step * slots : (step + 1) * slots] + arrived
            ).astype(jnp.bfloat16)


def combine_kernel(slot_ref, high_ref, low_ref, *refs):
    line_tokens, side = slot_ref.shape
    back_refs, (out_ref, taking, rows) = by_step(refs[:side]), refs[side:]
    slots, half = back_refs[0].shape
    slot_iota = lax.broadcasted_iota(jnp.int32, (line_tokens, slots), 1)
    for step in range(0, side, 2):
        columns = pl.ds(step * slots, 2 * slots)
        placed = [slot_ref[:, s : s + 1] == slot_iota for s in (step, step + 1)]
        for index, part_ref in enumerate((high_ref, low_ref)):
            taken = [
                jnp.where(here, part_ref[:, s : s + 1], 0.0)
                for here, s in zip(placed, (step, step + 1))
            ]
            taking[pl.ds(index * line_tokens, line_tokens), columns] = jnp.concatenate(
                taken, axis=1
            ).astype(jnp.bfloat16)
        for s in (step, step + 1):
            rows[pl.ds(s * slots, slots), :] = back_refs[s][...]
    tile = 256
    for column in range(0, half, tile):
        columns = pl.ds(column, tile)
        both = jnp.dot(taking[...], rows[:, columns], preferred_element_type=jnp.float32)
        total = (both[:line_tokens] + both[line_tokens:]).astype(jnp.bfloat16)
        out_ref[:, :, columns] = total.reshape(out_ref.shape[0], out_ref.shape[1], tile)


def split_in_two(value):
    high = value.astype(jnp.bfloat16)
    return high, (value - high.astype(jnp.float32)).astype(jnp.bfloat16)


def attention(q_latent, q_rope, cache_latent, cache_rope, lengths):
    scores = jnp.einsum("bhl,bjl->bhj", q_latent, cache_latent, preferred_element_type=jnp.float32)
    scores = scores + jnp.einsum(
        "bhr,brj->bhj", q_rope, cache_rope, preferred_element_type=jnp.float32
    )
    scores = scores * softmax_scale
    position = jnp.arange(cache_latent.shape[1], dtype=jnp.int32)
    live = position[None, None, :] < lengths[:, None, None]
    scores = jnp.where(live, scores, -jnp.inf)
    highest = jnp.max(scores, axis=2, keepdims=True)
    expo = jnp.where(live, jnp.exp(scores - highest), 0.0)
    attn_probs = (expo / jnp.sum(expo, axis=2, keepdims=True)).astype(jnp.bfloat16)
    attn_latent = jnp.einsum(
        "bhj,bjl->bhl", attn_probs, cache_latent, preferred_element_type=jnp.float32
    )
    return attn_latent.astype(jnp.bfloat16)


def local(
    hidden,
    routes,
    router_weight,
    gate_weight,
    up_weight,
    down_weight,
    q_latent,
    q_rope,
    cache_latent,
    cache_rope,
    lengths,
):
    token_count, top_count = routes.shape
    expert_count = lax.axis_size("ep")
    side = side_of(expert_count)
    capacity = min(token_count, 4 * token_count * top_count // expert_count)
    line_slots = side * capacity
    line_tokens = side * token_count
    half = hidden.shape[1]
    bf16, f32 = jnp.bfloat16, jnp.float32

    core = lax.axis_index("tp")
    place = lax.axis_index("ep")
    row, column = place // side, place % side
    first = jnp.where(core == 0, column, row)
    second = jnp.where(core == 0, row, column)
    side_iota = jnp.arange(side, dtype=jnp.int32)
    start = (core * half).astype(jnp.int32).reshape(1)

    expert_iota = jnp.arange(expert_count, dtype=jnp.int32)
    mask = jnp.sum((routes.T[:, :, None] == expert_iota).astype(f32), axis=0)
    partial_logits = jnp.dot(hidden, router_weight, preferred_element_type=f32)
    logits = partial_logits + swapped(partial_logits, "tp")
    chosen = jnp.where(mask > 0, jax.nn.sigmoid(logits), 0.0)
    gates = routed_scale * chosen / jnp.sum(chosen, axis=1, keepdims=True)

    ahead = (second + side_iota) % side
    experts = jnp.where(
        core == 0, ahead[None, :] * side + side_iota[:, None], side_iota[:, None] * side + ahead[None, :]
    )
    lanes = 128 * ((2 * side + 127) // 128)
    blank = jnp.full((side, lanes - 2 * side), -1, jnp.int32)
    wanted = jnp.concatenate([experts, expert_count + experts, blank], axis=1)
    source = jnp.arange(2 * expert_count, dtype=jnp.int32)
    gate_select = (wanted[:, None, :] == source[None, :, None]).astype(bf16)
    gate_parts = jnp.concatenate(split_in_two(gates), axis=1)
    gate_lanes = jnp.einsum("te,pec->ptc", gate_parts, gate_select, preferred_element_type=f32)
    message = jnp.concatenate(
        [jnp.broadcast_to(hidden[None], (side, token_count, half)), gate_lanes.astype(bf16)], axis=2
    )
    message, start = lax.optimization_barrier((message, start))
    line = lax.all_to_all(
        message, pair, 0, 0, axis_index_groups=first_groups(side), tiled=True
    )
    line_gates = line[:, :, half : half + 2 * side].reshape(line_tokens, 2 * side)
    gate_high, gate_low = line_gates[:, :side].astype(f32), line_gates[:, side:].astype(f32)

    picked = gate_high != 0
    token_iota = jnp.arange(line_tokens, dtype=jnp.int32)
    block_of = token_iota // token_count
    before = (token_iota[:, None] > token_iota[None, :]) & (block_of[:, None] == block_of[None, :])
    rank = jnp.dot(before.astype(bf16), picked.astype(bf16), preferred_element_type=f32)
    offset = ((first - block_of + side) % side) * capacity
    slot = jnp.where(picked, offset[:, None] + rank.astype(jnp.int32), -1)
    part_shape = jax.ShapeDtypeStruct((line_slots, half), bf16)
    rows = on_chip(select_kernel, (part_shape,) * side, (slot.T, line), "select")

    order = near_to_far(side)[1:]
    own, other = [rows[0]] + [None] * (side - 1), [None] * side
    for step in order:
        own[step] = shifted(rows[step], step, side)
    weights = fetched((gate_weight[0], up_weight[0], down_weight[0]), rows[0])
    other[0] = swapped(own[0], "tp")
    own[order[0]], *weights = lax.optimization_barrier((own[order[0]], *weights))
    for step in order:
        other[step] = swapped(own[step], "tp")
    gate_w, up_w, down_w = weights

    attn_latent = attention(q_latent, q_rope, cache_latent, cache_rope, lengths)

    all_slots = side * line_slots
    rows_scratch = pltpu.VMEM((all_slots, half), bf16)
    active, sent = on_chip(
        lambda *refs: expert_kernel(side, *refs),
        (
            jax.ShapeDtypeStruct((all_slots, gate_w.shape[1]), bf16),
            jax.ShapeDtypeStruct((side, side, capacity, half), bf16),
        ),
        (start, gate_w, up_w, down_w, *(own[s] for s in [0] + order), *(other[s] for s in [0] + order)),
        "expert",
        (rows_scratch, rows_scratch),
        16,
    )
    arrived = swapped(sent.reshape(all_slots, half), "tp")
    summed = on_chip(
        finish_kernel, (part_shape,) * side, (start, active, down_w, arrived), "finish"
    )

    back = [summed[0]] + [None] * (side - 1)
    for step in order:
        back[step] = shifted(summed[step], -step, side)
    line_shape = jax.ShapeDtypeStruct((side, token_count, half), bf16)
    weighted = on_chip(
        combine_kernel,
        line_shape,
        (slot, gate_high, gate_low, *(back[s] for s in [0] + order)),
        "combine",
        (pltpu.VMEM((2 * line_tokens, all_slots), bf16), rows_scratch),
    )
    shares = lax.all_to_all(
        weighted, pair, 0, 0, axis_index_groups=first_groups(side), tiled=True
    )
    moe_out = jnp.sum(shares.astype(f32), axis=0).astype(bf16)
    return (moe_out, attn_latent)


def solution(mesh):
    return jax.shard_map(
        local,
        mesh=mesh,
        in_specs=(
            P(("groups", "ep"), "tp"),
            P(("groups", "ep"), None),
            P("tp", None),
            P("ep", None, "tp"),
            P("ep", None, "tp"),
            P("ep", "tp", None),
            P(("groups", "ep"), "tp", None),
            P(("groups", "ep"), "tp", None),
            P(("groups", "ep"), None, None),
            P(("groups", "ep"), None, None),
            P(("groups", "ep")),
        ),
        out_specs=(P(("groups", "ep"), "tp"), P(("groups", "ep"), "tp", None)),
        check_vma=False,
    )
```

```python
import math

import jax
import jax.numpy as jnp
from jax import lax
from jax.experimental import pallas as pl
from jax.experimental.pallas import tpu as pltpu
from jax.sharding import PartitionSpec as P


softmax_scale = 192.0 ** (-0.5)
routed_scale = 2.5
pair = ("ep", "tp")


def side_of(devices):
    side = math.isqrt(devices)
    assert side * side == devices
    return side


def flat_index(first, second, core, side):
    row, column = (second, first) if core == 0 else (first, second)
    return (row * side + column) * 2 + core


def first_groups(side):
    return [
        [flat_index(first, second, core, side) for first in range(side)]
        for core in range(2)
        for second in range(side)
    ]


def shifted(value, shift, side):
    moves = []
    for core in range(2):
        for first in range(side):
            for second in range(side):
                target = (second + shift) % side
                moves.append(
                    (flat_index(first, second, core, side), flat_index(first, target, core, side))
                )
    return lax.ppermute(value, pair, moves)


def swapped(value, axis):
    return lax.ppermute(value, axis, [(0, 1), (1, 0)])


def on_chip(kernel, out_shapes, operands, scratch=(), limit=16):
    return pl.pallas_call(
        kernel,
        out_shape=out_shapes,
        in_specs=[
            pl.BlockSpec(memory_space=pltpu.SMEM if a.ndim == 1 else pltpu.VMEM) for a in operands
        ],
        out_specs=jax.tree.map(lambda _: pl.BlockSpec(memory_space=pltpu.VMEM), out_shapes),
        scratch_shapes=list(scratch),
        compiler_params=pltpu.CompilerParams(vmem_limit_bytes=limit * 1024 * 1024),
    )(*operands)


def message_kernel(place_ref, hidden_ref, own_ref, other_ref, mask_ref, message_ref):
    side, _, width = message_ref.shape
    half = hidden_ref.shape[1]
    lanes = width - half
    expert_count = mask_ref.shape[1]
    core, second = place_ref[1], place_ref[2]
    chosen = jnp.where(mask_ref[...] > 0, jax.nn.sigmoid(own_ref[...] + other_ref[...]), 0.0)
    gates = routed_scale * chosen / jnp.sum(chosen, axis=1, keepdims=True)
    parts = jnp.concatenate([part.astype(jnp.float32) for part in split_in_two(gates)], axis=1)
    shape = (2 * expert_count, lanes)
    source = lax.broadcasted_iota(jnp.int32, shape, 0)
    lane = lax.broadcasted_iota(jnp.int32, shape, 1)
    low = (lane >= side).astype(jnp.int32)
    ahead = lax.rem(lane - low * side + second, side)
    scale = jnp.where(core == 0, side, 1)
    base = ahead * scale + low * expert_count
    for first in range(side):
        wanted = base + first * jnp.where(core == 0, 1, side)
        select = jnp.where((lane < 2 * side) & (wanted == source), 1.0, 0.0)
        picked = jnp.dot(
            parts.astype(jnp.bfloat16), select.astype(jnp.bfloat16), preferred_element_type=jnp.float32
        )
        message_ref[first, :, pl.ds(0, half)] = hidden_ref[...]
        message_ref[first, :, pl.ds(half, lanes)] = picked.astype(jnp.bfloat16)


def fetch_kernel(*refs):
    sources, (slot_ref, high_ref, low_ref, _), refs = refs[:3], refs[3:7], refs[7:]
    targets, taking, sems = refs[:3], refs[3], refs[4:]
    copies = [pltpu.make_async_copy(s, t, m) for s, t, m in zip(sources, targets, sems)]
    for copy in copies:
        copy.start()
    line_tokens, side = slot_ref.shape
    slots = taking.shape[1] // side
    slot_iota = lax.broadcasted_iota(jnp.int32, (line_tokens, slots), 1)
    steps = far_to_near(side)
    for place in range(0, side, 2):
        columns = pl.ds(place * slots, 2 * slots)
        pair_of = steps[place : place + 2]
        for index, part_ref in enumerate((high_ref, low_ref)):
            taken = [
                jnp.where(slot_ref[:, s : s + 1] == slot_iota, part_ref[:, s : s + 1], 0.0)
                for s in pair_of
            ]
            taking[pl.ds(index * line_tokens, line_tokens), columns] = jnp.concatenate(
                taken, axis=1
            ).astype(jnp.bfloat16)
    for copy in copies:
        copy.wait()


def fetched(arrays, slot, high, low, after):
    line_tokens, side = slot.shape
    taking_shape = (2 * line_tokens, side * after.shape[0])
    vmem = pl.BlockSpec(memory_space=pltpu.VMEM)
    return pl.pallas_call(
        fetch_kernel,
        out_shape=tuple(pltpu.VMEM(a.shape, a.dtype) for a in arrays)
        + (jax.ShapeDtypeStruct(taking_shape, jnp.bfloat16),),
        in_specs=[pl.BlockSpec(memory_space=pltpu.HBM)] * 3
        + [vmem] * 3
        + [pl.BlockSpec(memory_space=pl.ANY)],
        out_specs=(vmem,) * 4,
        scratch_shapes=[pltpu.SemaphoreType.DMA] * len(arrays),
        compiler_params=pltpu.CompilerParams(vmem_limit_bytes=42 * 1024 * 1024),
        name="fetch_weights",
    )(*arrays, slot, high, low, after)


def select_kernel(slot_ref, line_ref, *part_refs):
    side, line_tokens = slot_ref.shape
    slots, half = part_refs[0].shape
    tokens = line_ref[:, :, :half].reshape(line_tokens, half)
    slot_iota = lax.broadcasted_iota(jnp.int32, (slots, line_tokens), 0)
    for step in range(side):
        placing = (slot_ref[step : step + 1, :] == slot_iota).astype(jnp.float32).astype(jnp.bfloat16)
        rows = jnp.dot(placing, tokens, preferred_element_type=jnp.float32)
        part_refs[step][...] = rows.astype(jnp.bfloat16)


def far_to_near(side):
    return sorted(range(side), key=lambda step: (-min(step, side - step), step))


def by_step(parts):
    steps = far_to_near(len(parts))
    return [parts[steps.index(step)] for step in range(len(parts))]


def expert_kernel(side, start_ref, gate_ref, up_ref, down_ref, *refs):
    own_refs, other_refs = by_step(refs[:side]), by_step(refs[side : 2 * side])
    active_ref, sent_ref, own, other = refs[2 * side :]
    early = early_parts(side)
    slots, half = own_refs[0].shape
    capacity = slots // side
    width = gate_ref.shape[1]
    for step in range(side):
        rows = pl.ds(step * slots, slots)
        own[rows, :] = own_refs[step][...]
        for block in range(side):
            other[pl.ds(step * slots + block * capacity, capacity), :] = other_refs[block][
                pl.ds(step * capacity, capacity), :
            ]
    mine = pl.multiple_of(start_ref[0], 256)
    theirs = pl.multiple_of(half - mine, 256)

    def product(weight_ref, columns):
        return jnp.dot(
            own[...], weight_ref[pl.ds(mine, half), columns], preferred_element_type=jnp.float32
        ) + jnp.dot(
            other[...], weight_ref[pl.ds(theirs, half), columns], preferred_element_type=jnp.float32
        )

    tile = 256
    for column in range(0, width, tile):
        columns = pl.ds(column, tile)
        gate_part = product(gate_ref, columns)
        up_part = product(up_ref, columns)
        active_ref[:, columns] = (jax.nn.silu(gate_part) * up_part).astype(jnp.bfloat16)
    send_blocks(early, theirs, active_ref, down_ref, sent_ref)


def early_parts(side):
    return far_to_near(side)[: side // 2 - 1]


def late_parts(side):
    return far_to_near(side)[side // 2 - 1 :]


def send_blocks(blocks, theirs, active_ref, down_ref, sent_ref):
    count, slots, half = sent_ref.shape
    width = active_ref.shape[1]
    side = active_ref.shape[0] // slots
    capacity = slots // side
    active = active_ref[...].reshape(side, side, capacity, width)
    rows = jnp.concatenate([active[:, block].reshape(slots, width) for block in blocks], axis=0)
    tile = 256
    for column in range(0, half, tile):
        weight = down_ref[:, pl.ds(pl.multiple_of(theirs + column, 256), tile)]
        sent = jnp.dot(rows, weight, preferred_element_type=jnp.float32).astype(jnp.bfloat16)
        sent_ref[:, :, pl.ds(column, tile)] = sent.reshape(count, slots, tile)


def late_kernel(side, start_ref, active_ref, down_ref, sent_ref):
    theirs = pl.multiple_of(sent_ref.shape[2] - start_ref[0], 256)
    send_blocks(late_parts(side), theirs, active_ref, down_ref, sent_ref)


def finish_kernel(steps, start_ref, active_ref, down_ref, arrived_ref, *part_refs):
    slots, half = part_refs[0].shape
    mine = start_ref[0]
    rows = jnp.concatenate([active_ref[pl.ds(step * slots, slots), :] for step in steps], axis=0)
    tile = 256
    for column in range(0, half, tile):
        columns = pl.ds(column, tile)
        weight = down_ref[:, pl.ds(pl.multiple_of(mine + column, 256), tile)]
        kept = jnp.dot(rows, weight, preferred_element_type=jnp.float32)
        for index in range(len(steps)):
            arrived = arrived_ref[index, :, columns].astype(jnp.float32)
            part_refs[index][:, columns] = (
                kept[index * slots : (index + 1) * slots] + arrived
            ).astype(jnp.bfloat16)


def gather_kernel(place, taking_ref, *refs):
    back_refs, (out_ref, rows) = refs[:-2], refs[-2:]
    slots, half = back_refs[0].shape
    depth = len(back_refs) * slots
    for index, back_ref in enumerate(back_refs):
        rows[pl.ds(index * slots, slots), :] = back_ref[...]
    taking = taking_ref[:, place * slots : place * slots + depth]
    line_tokens = taking.shape[0] // 2
    tile = 256
    for column in range(0, half, tile):
        columns = pl.ds(column, tile)
        both = jnp.dot(taking, rows[:, columns], preferred_element_type=jnp.float32)
        out_ref[:, columns] = both[:line_tokens] + both[line_tokens:]


def combine_kernel(place, taking_ref, sofar_ref, *refs):
    back_refs, (out_ref, rows) = refs[:-2], refs[-2:]
    slots, half = back_refs[0].shape
    depth = len(back_refs) * slots
    for index, back_ref in enumerate(back_refs):
        rows[pl.ds(index * slots, slots), :] = back_ref[...]
    taking = taking_ref[:, place * slots : place * slots + depth]
    line_tokens = taking.shape[0] // 2
    tile = 256
    for column in range(0, half, tile):
        columns = pl.ds(column, tile)
        both = jnp.dot(taking, rows[:, columns], preferred_element_type=jnp.float32)
        total = sofar_ref[:, columns] + both[:line_tokens] + both[line_tokens:]
        out_ref[:, :, columns] = total.astype(jnp.bfloat16).reshape(
            out_ref.shape[0], out_ref.shape[1], tile
        )


def split_in_two(value):
    high = value.astype(jnp.bfloat16)
    return high, (value - high.astype(jnp.float32)).astype(jnp.bfloat16)


def attention(q_latent, q_rope, cache_latent, cache_rope, lengths):
    scores = jnp.einsum("bhl,bjl->bhj", q_latent, cache_latent, preferred_element_type=jnp.float32)
    scores = scores + jnp.einsum(
        "bhr,brj->bhj", q_rope, cache_rope, preferred_element_type=jnp.float32
    )
    scores = scores * softmax_scale
    position = jnp.arange(cache_latent.shape[1], dtype=jnp.int32)
    live = position[None, None, :] < lengths[:, None, None]
    scores = jnp.where(live, scores, -jnp.inf)
    highest = jnp.max(scores, axis=2, keepdims=True)
    expo = jnp.where(live, jnp.exp(scores - highest), 0.0)
    attn_probs = (expo / jnp.sum(expo, axis=2, keepdims=True)).astype(jnp.bfloat16)
    attn_latent = jnp.einsum(
        "bhj,bjl->bhl", attn_probs, cache_latent, preferred_element_type=jnp.float32
    )
    return attn_latent.astype(jnp.bfloat16)


def local(
    hidden,
    routes,
    router_weight,
    gate_weight,
    up_weight,
    down_weight,
    q_latent,
    q_rope,
    cache_latent,
    cache_rope,
    lengths,
):
    token_count, top_count = routes.shape
    expert_count = lax.axis_size("ep")
    side = side_of(expert_count)
    capacity = min(token_count, 4 * token_count * top_count // expert_count)
    line_slots = side * capacity
    line_tokens = side * token_count
    half = hidden.shape[1]
    bf16, f32 = jnp.bfloat16, jnp.float32

    core = lax.axis_index("tp")
    place = lax.axis_index("ep")
    row, column = place // side, place % side
    first = jnp.where(core == 0, column, row)
    second = jnp.where(core == 0, row, column)
    start = jnp.stack([core * half, core, second]).astype(jnp.int32)

    expert_iota = jnp.arange(expert_count, dtype=jnp.int32)
    mask = jnp.sum((routes.T[:, :, None] == expert_iota).astype(f32), axis=0)
    partial_logits = jnp.dot(hidden, router_weight, preferred_element_type=f32)
    other_logits = swapped(partial_logits, "tp")

    lanes = 128 * ((2 * side + 127) // 128)
    message = on_chip(
        message_kernel,
        jax.ShapeDtypeStruct((side, token_count, half + lanes), bf16),
        (start, hidden, partial_logits, other_logits, mask),
    )
    message, start = lax.optimization_barrier((message, start))
    line = lax.all_to_all(
        message, pair, 0, 0, axis_index_groups=first_groups(side), tiled=True
    )
    line_gates = line[:, :, half : half + 2 * side].reshape(line_tokens, 2 * side)
    gate_high, gate_low = line_gates[:, :side].astype(f32), line_gates[:, side:].astype(f32)

    picked = gate_high != 0
    token_iota = jnp.arange(line_tokens, dtype=jnp.int32)
    block_of = token_iota // token_count
    before = (token_iota[:, None] > token_iota[None, :]) & (block_of[:, None] == block_of[None, :])
    rank = jnp.dot(before.astype(bf16), picked.astype(bf16), preferred_element_type=f32)
    offset = ((first - block_of + side) % side) * capacity
    slot = jnp.where(picked, offset[:, None] + rank.astype(jnp.int32), -1)
    part_shape = jax.ShapeDtypeStruct((line_slots, half), bf16)
    rows = on_chip(select_kernel, (part_shape,) * side, (slot.T, line))

    order = [step for step in far_to_near(side) if step]
    own, other = [rows[0]] + [None] * (side - 1), [None] * side
    for step in order:
        own[step] = shifted(rows[step], step, side)
    weights = (gate_weight[0], up_weight[0], down_weight[0])
    *weights, taking = fetched(weights, slot, gate_high, gate_low, rows[0])
    other[0] = swapped(own[0], "tp")
    own[order[0]], *weights = lax.optimization_barrier((own[order[0]], *weights))
    for step in order:
        other[step] = swapped(own[step], "tp")
    gate_w, up_w, down_w = weights

    attn_latent = attention(q_latent, q_rope, cache_latent, cache_rope, lengths)

    all_slots = side * line_slots
    rows_scratch = pltpu.VMEM((all_slots, half), bf16)
    early, late = early_parts(side), late_parts(side)
    steps = far_to_near(side)
    active, sent = on_chip(
        lambda *refs: expert_kernel(side, *refs),
        (
            jax.ShapeDtypeStruct((all_slots, gate_w.shape[1]), bf16),
            jax.ShapeDtypeStruct((len(early), line_slots, half), bf16),
        ),
        (start, gate_w, up_w, down_w, *(own[s] for s in steps), *(other[s] for s in steps)),
        (rows_scratch, rows_scratch),
        16,
    )
    early_arrived = swapped(sent, "tp")
    late_sent = on_chip(
        lambda *refs: late_kernel(side, *refs),
        jax.ShapeDtypeStruct((len(late), line_slots, half), bf16),
        (start, active, down_w),
    )
    late_arrived = swapped(late_sent, "tp")
    summed = {}
    for steps_of, arrived in ((early, early_arrived), (late, late_arrived)):
        parts = on_chip(
            lambda *refs, steps_of=steps_of: finish_kernel(steps_of, *refs),
            (part_shape,) * len(steps_of),
            (start, active, down_w, arrived),
        )
        summed.update(zip(steps_of, parts))

    back = {0: summed[0]}
    for step in order:
        back[step] = shifted(summed[step], -step, side)
    cut = side // 2
    half_scratch = pltpu.VMEM((cut * line_slots, half), bf16)
    sofar = on_chip(
        lambda *refs: gather_kernel(0, *refs),
        jax.ShapeDtypeStruct((line_tokens, half), f32),
        (taking, *(back[s] for s in steps[:cut])),
        (half_scratch,),
    )
    weighted = on_chip(
        lambda *refs: combine_kernel(cut, *refs),
        jax.ShapeDtypeStruct((side, token_count, half), bf16),
        (taking, sofar, *(back[s] for s in steps[cut:])),
        (half_scratch,),
    )
    shares = lax.all_to_all(
        weighted, pair, 0, 0, axis_index_groups=first_groups(side), tiled=True
    )
    moe_out = jnp.sum(shares.astype(f32), axis=0).astype(bf16)
    return (moe_out, attn_latent)


def solution(mesh):
    return jax.shard_map(
        local,
        mesh=mesh,
        in_specs=(
            P(("groups", "ep"), "tp"),
            P(("groups", "ep"), None),
            P("tp", None),
            P("ep", None, "tp"),
            P("ep", None, "tp"),
            P("ep", "tp", None),
            P(("groups", "ep"), "tp", None),
            P(("groups", "ep"), "tp", None),
            P(("groups", "ep"), None, None),
            P(("groups", "ep"), None, None),
            P(("groups", "ep")),
        ),
        out_specs=(P(("groups", "ep"), "tp"), P(("groups", "ep"), "tp", None)),
        check_vma=False,
    )
```

```python
import math

import jax
import jax.numpy as jnp
from jax import lax
from jax.experimental import pallas as pl
from jax.experimental.pallas import tpu as pltpu
from jax.sharding import PartitionSpec as P


softmax_scale = 192.0 ** (-0.5)
routed_scale = 2.5
pair = ("ep", "tp")


def side_of(devices):
    side = math.isqrt(devices)
    assert side * side == devices
    return side


def flat_index(first, second, core, side):
    row, column = (second, first) if core == 0 else (first, second)
    return (row * side + column) * 2 + core


def first_groups(side):
    return [
        [flat_index(first, second, core, side) for first in range(side)]
        for core in range(2)
        for second in range(side)
    ]


def shifted(value, shift, side):
    moves = []
    for core in range(2):
        for first in range(side):
            for second in range(side):
                target = (second + shift) % side
                moves.append(
                    (flat_index(first, second, core, side), flat_index(first, target, core, side))
                )
    return lax.ppermute(value, pair, moves)


def swapped(value, axis):
    return lax.ppermute(value, axis, [(0, 1), (1, 0)])


def on_chip(kernel, out_shapes, operands, scratch=(), limit=16):
    return pl.pallas_call(
        kernel,
        out_shape=out_shapes,
        in_specs=[
            pl.BlockSpec(memory_space=pltpu.SMEM if a.ndim == 1 else pltpu.VMEM) for a in operands
        ],
        out_specs=jax.tree.map(lambda _: pl.BlockSpec(memory_space=pltpu.VMEM), out_shapes),
        scratch_shapes=list(scratch),
        compiler_params=pltpu.CompilerParams(vmem_limit_bytes=limit * 1024 * 1024),
    )(*operands)


def message_kernel(place_ref, hidden_ref, own_ref, other_ref, mask_ref, message_ref, sum_ref):
    side, _, width = message_ref.shape
    half = hidden_ref.shape[1]
    lanes = width - half
    expert_count = mask_ref.shape[1]
    core, second = place_ref[1], place_ref[2]
    chosen = jnp.where(mask_ref[...] > 0, jax.nn.sigmoid(own_ref[...] + other_ref[...]), 0.0)
    affinity_sum = jnp.sum(chosen, axis=1, keepdims=True)
    sum_ref[...] = affinity_sum
    gates = jnp.where(affinity_sum > 0, routed_scale * chosen / affinity_sum, 0.0)
    parts = jnp.concatenate([part.astype(jnp.float32) for part in split_in_two(gates)], axis=1)
    shape = (2 * expert_count, side * lanes)
    source = lax.broadcasted_iota(jnp.int32, shape, 0)
    column = lax.broadcasted_iota(jnp.int32, shape, 1)
    first = lax.div(column, lanes)
    lane = column - first * lanes
    low = (lane >= side).astype(jnp.int32)
    ahead = lax.rem(lane - low * side + second, side)
    wanted = jnp.where(core == 0, ahead * side + first, first * side + ahead) + low * expert_count
    select = jnp.where((lane < 2 * side) & (wanted == source), 1.0, 0.0).astype(jnp.bfloat16)
    picked = jnp.dot(parts.astype(jnp.bfloat16), select, preferred_element_type=jnp.float32)
    picked = picked.astype(jnp.bfloat16)
    for first in range(side):
        message_ref[first, :, pl.ds(0, half)] = hidden_ref[...]
        message_ref[first, :, pl.ds(half, lanes)] = picked[:, first * lanes : (first + 1) * lanes]


def fetch_kernel(side, *refs):
    sources, (slot_ref, gate_ref, _), refs = refs[:3], refs[3:6], refs[6:]
    targets, taking, sems = refs[:3], refs[3], refs[4:]
    copies = [pltpu.make_async_copy(s, t, m) for s, t, m in zip(sources, targets, sems)]
    for copy in copies:
        copy.start()
    line_tokens = slot_ref.shape[0]
    slots = taking.shape[1] // side
    slot_iota = lax.broadcasted_iota(jnp.int32, (line_tokens, slots), 1)
    steps = far_to_near(side)
    for place in range(0, side, 2):
        columns = pl.ds(place * slots, 2 * slots)
        pair_of = steps[place : place + 2]
        for index in range(2):
            taken = [
                jnp.where(
                    slot_ref[:, s : s + 1] == slot_iota,
                    gate_ref[:, index * side + s : index * side + s + 1],
                    0.0,
                )
                for s in pair_of
            ]
            taking[pl.ds(index * line_tokens, line_tokens), columns] = jnp.concatenate(
                taken, axis=1
            ).astype(jnp.bfloat16)
    for copy in copies:
        copy.wait()


def fetched(arrays, side, slot, gates, after):
    line_tokens = slot.shape[0]
    taking_shape = (2 * line_tokens, side * after.shape[0])
    vmem = pl.BlockSpec(memory_space=pltpu.VMEM)
    return pl.pallas_call(
        lambda *refs: fetch_kernel(side, *refs),
        out_shape=tuple(pltpu.VMEM(a.shape, a.dtype) for a in arrays)
        + (jax.ShapeDtypeStruct(taking_shape, jnp.bfloat16),),
        in_specs=[pl.BlockSpec(memory_space=pltpu.HBM)] * 3
        + [vmem] * 2
        + [pl.BlockSpec(memory_space=pl.ANY)],
        out_specs=(vmem,) * 4,
        scratch_shapes=[pltpu.SemaphoreType.DMA] * len(arrays),
        compiler_params=pltpu.CompilerParams(vmem_limit_bytes=42 * 1024 * 1024),
        name="fetch_weights",
    )(*arrays, slot, gates, after)


def select_kernel(capacity, place_ref, line_ref, *refs):
    part_refs, (slot_ref, gate_ref) = refs[:-2], refs[-2:]
    side, token_count, width = line_ref.shape
    slots, half = part_refs[0].shape
    line_tokens = side * token_count
    first = place_ref[3]
    gates = line_ref[:, :, pl.ds(half, width - half)].reshape(line_tokens, width - half)
    gates = gates.astype(jnp.float32)
    gate_ref[...] = gates
    shape = (line_tokens, line_tokens)
    later = lax.broadcasted_iota(jnp.int32, shape, 0)
    earlier = lax.broadcasted_iota(jnp.int32, shape, 1)
    same = lax.div(later, token_count) == lax.div(earlier, token_count)
    before = jnp.where(same & (later > earlier), 1.0, 0.0).astype(jnp.bfloat16)
    picked = jnp.where(gates != 0, 1.0, 0.0).astype(jnp.bfloat16)
    rank = jnp.dot(before, picked, preferred_element_type=jnp.float32)
    block = lax.div(lax.broadcasted_iota(jnp.int32, gates.shape, 0), token_count)
    offset = lax.rem(first - block + side, side) * capacity
    slot = jnp.where(gates != 0, offset.astype(jnp.float32) + rank, -1.0)
    slot_ref[...] = slot.astype(jnp.int32)
    slot_rows = jnp.transpose(slot).astype(jnp.int32)
    tokens = line_ref[:, :, pl.ds(0, half)].reshape(line_tokens, half)
    slot_iota = lax.broadcasted_iota(jnp.int32, (slots, line_tokens), 0)
    for step in range(side):
        placing = jnp.where(slot_rows[step : step + 1, :] == slot_iota, 1.0, 0.0)
        rows = jnp.dot(placing.astype(jnp.bfloat16), tokens, preferred_element_type=jnp.float32)
        part_refs[step][...] = rows.astype(jnp.bfloat16)


def far_to_near(side):
    return sorted(range(side), key=lambda step: (-min(step, side - step), step))


def by_step(parts):
    steps = far_to_near(len(parts))
    return [parts[steps.index(step)] for step in range(len(parts))]


def expert_kernel(side, start_ref, gate_ref, up_ref, down_ref, *refs):
    own_refs, other_refs = by_step(refs[:side]), by_step(refs[side : 2 * side])
    active_ref, sent_ref, own, other = refs[2 * side :]
    early = early_parts(side)
    slots, half = own_refs[0].shape
    capacity = slots // side
    width = gate_ref.shape[1]
    for step in range(side):
        rows = pl.ds(step * slots, slots)
        own[rows, :] = own_refs[step][...]
        for block in range(side):
            other[pl.ds(step * slots + block * capacity, capacity), :] = other_refs[block][
                pl.ds(step * capacity, capacity), :
            ]
    mine = pl.multiple_of(start_ref[0], 256)
    theirs = pl.multiple_of(half - mine, 256)

    def product(weight_ref, columns):
        return jnp.dot(
            own[...], weight_ref[pl.ds(mine, half), columns], preferred_element_type=jnp.float32
        ) + jnp.dot(
            other[...], weight_ref[pl.ds(theirs, half), columns], preferred_element_type=jnp.float32
        )

    tile = 256
    for column in range(0, width, tile):
        columns = pl.ds(column, tile)
        gate_part = product(gate_ref, columns)
        up_part = product(up_ref, columns)
        active_ref[:, columns] = (jax.nn.silu(gate_part) * up_part).astype(jnp.bfloat16)
    send_blocks(early, theirs, active_ref, down_ref, sent_ref)


def early_parts(side):
    return far_to_near(side)[: side // 2 - 1]


def late_parts(side):
    return far_to_near(side)[side // 2 - 1 :]


def send_blocks(blocks, theirs, active_ref, down_ref, sent_ref):
    count, slots, half = sent_ref.shape
    width = active_ref.shape[1]
    side = active_ref.shape[0] // slots
    capacity = slots // side
    active = active_ref[...].reshape(side, side, capacity, width)
    rows = jnp.concatenate([active[:, block].reshape(slots, width) for block in blocks], axis=0)
    tile = 256
    for column in range(0, half, tile):
        weight = down_ref[:, pl.ds(pl.multiple_of(theirs + column, 256), tile)]
        sent = jnp.dot(rows, weight, preferred_element_type=jnp.float32).astype(jnp.bfloat16)
        sent_ref[:, :, pl.ds(column, tile)] = sent.reshape(count, slots, tile)


def late_kernel(side, start_ref, active_ref, down_ref, sent_ref):
    theirs = pl.multiple_of(sent_ref.shape[2] - start_ref[0], 256)
    send_blocks(late_parts(side), theirs, active_ref, down_ref, sent_ref)


def finish_kernel(steps, start_ref, active_ref, down_ref, arrived_ref, *part_refs):
    slots, half = part_refs[0].shape
    mine = start_ref[0]
    rows = jnp.concatenate([active_ref[pl.ds(step * slots, slots), :] for step in steps], axis=0)
    tile = 256
    for column in range(0, half, tile):
        columns = pl.ds(column, tile)
        weight = down_ref[:, pl.ds(pl.multiple_of(mine + column, 256), tile)]
        kept = jnp.dot(rows, weight, preferred_element_type=jnp.float32)
        for index in range(len(steps)):
            arrived = arrived_ref[index, :, columns].astype(jnp.float32)
            part_refs[index][:, columns] = (
                kept[index * slots : (index + 1) * slots] + arrived
            ).astype(jnp.bfloat16)


def gather_kernel(place, taking_ref, *refs):
    back_refs, (out_ref, rows) = refs[:-2], refs[-2:]
    slots, half = back_refs[0].shape
    depth = len(back_refs) * slots
    for index, back_ref in enumerate(back_refs):
        rows[pl.ds(index * slots, slots), :] = back_ref[...]
    taking = taking_ref[:, place * slots : place * slots + depth]
    line_tokens = taking.shape[0] // 2
    tile = 256
    for column in range(0, half, tile):
        columns = pl.ds(column, tile)
        both = jnp.dot(taking, rows[:, columns], preferred_element_type=jnp.float32)
        out_ref[:, columns] = both[:line_tokens] + both[line_tokens:]


def combine_kernel(place, taking_ref, sofar_ref, *refs):
    refs = refs[1:]
    back_refs, (out_ref, rows) = refs[:-2], refs[-2:]
    slots, half = back_refs[0].shape
    depth = len(back_refs) * slots
    for index, back_ref in enumerate(back_refs):
        rows[pl.ds(index * slots, slots), :] = back_ref[...]
    taking = taking_ref[:, place * slots : place * slots + depth]
    line_tokens = taking.shape[0] // 2
    tile = 256
    for column in range(0, half, tile):
        columns = pl.ds(column, tile)
        both = jnp.dot(taking, rows[:, columns], preferred_element_type=jnp.float32)
        total = sofar_ref[:, columns] + both[:line_tokens] + both[line_tokens:]
        out_ref[:, :, columns] = total.astype(jnp.bfloat16).reshape(
            out_ref.shape[0], out_ref.shape[1], tile
        )


def total_kernel(sum_ref, share_ref, out_ref):
    total = share_ref[0].astype(jnp.float32)
    for step in range(1, share_ref.shape[0]):
        total = total + share_ref[step].astype(jnp.float32)
    out_ref[...] = jnp.where(sum_ref[...] > 0, total, jnp.nan).astype(out_ref.dtype)


def split_in_two(value):
    high = value.astype(jnp.bfloat16)
    return high, (value - high.astype(jnp.float32)).astype(jnp.bfloat16)


def attention(q_latent, q_rope, cache_latent, cache_rope, lengths):
    scores = jnp.einsum("bhl,bjl->bhj", q_latent, cache_latent, preferred_element_type=jnp.float32)
    scores = scores + jnp.einsum(
        "bhr,brj->bhj", q_rope, cache_rope, preferred_element_type=jnp.float32
    )
    scores = scores * softmax_scale
    position = jnp.arange(cache_latent.shape[1], dtype=jnp.int32)
    live = position[None, None, :] < lengths[:, None, None]
    scores = jnp.where(live, scores, -jnp.inf)
    highest = jnp.max(scores, axis=2, keepdims=True)
    expo = jnp.where(live, jnp.exp(scores - highest), 0.0)
    attn_probs = (expo / jnp.sum(expo, axis=2, keepdims=True)).astype(jnp.bfloat16)
    attn_latent = jnp.einsum(
        "bhj,bjl->bhl", attn_probs, cache_latent, preferred_element_type=jnp.float32
    )
    return attn_latent.astype(jnp.bfloat16)


def local(
    hidden,
    routes,
    router_weight,
    gate_weight,
    up_weight,
    down_weight,
    q_latent,
    q_rope,
    cache_latent,
    cache_rope,
    lengths,
):
    token_count, top_count = routes.shape
    expert_count = lax.axis_size("ep")
    side = side_of(expert_count)
    capacity = min(token_count, 4 * token_count * top_count // expert_count)
    line_slots = side * capacity
    line_tokens = side * token_count
    half = hidden.shape[1]
    bf16, f32 = jnp.bfloat16, jnp.float32

    core = lax.axis_index("tp")
    place = lax.axis_index("ep")
    row, column = place // side, place % side
    first = jnp.where(core == 0, column, row)
    second = jnp.where(core == 0, row, column)
    start = jnp.stack([core * half, core, second, first]).astype(jnp.int32)

    expert_iota = jnp.arange(expert_count, dtype=jnp.int32)
    mask = jnp.sum((routes.T[:, :, None] == expert_iota).astype(f32), axis=0)
    partial_logits = jnp.dot(hidden, router_weight, preferred_element_type=f32)
    other_logits = swapped(partial_logits, "tp")

    lanes = 128 * ((2 * side + 127) // 128)
    message, affinity_sum = on_chip(
        message_kernel,
        (
            jax.ShapeDtypeStruct((side, token_count, half + lanes), bf16),
            jax.ShapeDtypeStruct((token_count, 1), f32),
        ),
        (start, hidden, partial_logits, other_logits, mask),
    )
    line = lax.all_to_all(
        message, pair, 0, 0, axis_index_groups=first_groups(side), tiled=True
    )
    part_shape = jax.ShapeDtypeStruct((line_slots, half), bf16)
    *rows, slot, line_gates = on_chip(
        lambda *refs: select_kernel(capacity, *refs),
        (part_shape,) * side
        + (
            jax.ShapeDtypeStruct((line_tokens, lanes), jnp.int32),
            jax.ShapeDtypeStruct((line_tokens, lanes), f32),
        ),
        (start, line),
    )

    order = [step for step in far_to_near(side) if step]
    own, other = [rows[0]] + [None] * (side - 1), [None] * side
    for step in order:
        own[step] = shifted(rows[step], step, side)
    weights = (gate_weight[0], up_weight[0], down_weight[0])
    *weights, taking = fetched(weights, side, slot, line_gates, rows[0])
    other[0] = swapped(own[0], "tp")
    own[order[0]], *weights = lax.optimization_barrier((own[order[0]], *weights))
    for step in order:
        other[step] = swapped(own[step], "tp")
    gate_w, up_w, down_w = weights

    attn_latent = attention(q_latent, q_rope, cache_latent, cache_rope, lengths)

    all_slots = side * line_slots
    rows_scratch = pltpu.VMEM((all_slots, half), bf16)
    early, late = early_parts(side), late_parts(side)
    steps = far_to_near(side)
    active, sent = on_chip(
        lambda *refs: expert_kernel(side, *refs),
        (
            jax.ShapeDtypeStruct((all_slots, gate_w.shape[1]), bf16),
            jax.ShapeDtypeStruct((len(early), line_slots, half), bf16),
        ),
        (start, gate_w, up_w, down_w, *(own[s] for s in steps), *(other[s] for s in steps)),
        (rows_scratch, rows_scratch),
        16,
    )
    early_arrived = swapped(sent, "tp")
    late_sent = on_chip(
        lambda *refs: late_kernel(side, *refs),
        jax.ShapeDtypeStruct((len(late), line_slots, half), bf16),
        (start, active, down_w),
    )
    late_arrived = swapped(late_sent, "tp")
    summed = {}
    for steps_of, arrived in ((early, early_arrived), (late, late_arrived)):
        parts = on_chip(
            lambda *refs, steps_of=steps_of: finish_kernel(steps_of, *refs),
            (part_shape,) * len(steps_of),
            (start, active, down_w, arrived),
        )
        summed.update(zip(steps_of, parts))

    back = {0: summed[0]}
    for step in order:
        back[step] = shifted(summed[step], -step, side)
    cut = side // 2
    half_scratch = pltpu.VMEM((cut * line_slots, half), bf16)
    sofar = on_chip(
        lambda *refs: gather_kernel(0, *refs),
        jax.ShapeDtypeStruct((line_tokens, half), f32),
        (taking, *(back[s] for s in steps[:cut])),
        (half_scratch,),
    )
    weighted = on_chip(
        lambda *refs: combine_kernel(cut, *refs),
        jax.ShapeDtypeStruct((side, token_count, half), bf16),
        (taking, sofar, attn_latent, *(back[s] for s in steps[cut:])),
        (half_scratch,),
    )
    shares = lax.all_to_all(
        weighted, pair, 0, 0, axis_index_groups=first_groups(side), tiled=True
    )
    moe_out = on_chip(
        total_kernel, jax.ShapeDtypeStruct((token_count, half), bf16), (affinity_sum, shares)
    )
    return (moe_out, attn_latent)


def solution(mesh):
    return jax.shard_map(
        local,
        mesh=mesh,
        in_specs=(
            P(("groups", "ep"), "tp"),
            P(("groups", "ep"), None),
            P("tp", None),
            P("ep", None, "tp"),
            P("ep", None, "tp"),
            P("ep", "tp", None),
            P(("groups", "ep"), "tp", None),
            P(("groups", "ep"), "tp", None),
            P(("groups", "ep"), None, None),
            P(("groups", "ep"), None, None),
            P(("groups", "ep")),
        ),
        out_specs=(P(("groups", "ep"), "tp"), P(("groups", "ep"), "tp", None)),
        check_vma=False,
    )
```

```python
import math

import jax
import jax.numpy as jnp
from jax import lax
from jax.experimental import pallas as pl
from jax.experimental.pallas import tpu as pltpu
from jax.sharding import PartitionSpec as P


softmax_scale = 192.0 ** (-0.5)
routed_scale = 2.5
pair = ("ep", "tp")


def side_of(devices):
    side = math.isqrt(devices)
    assert side * side == devices
    return side


def flat_index(first, second, core, side):
    row, column = (second, first) if core == 0 else (first, second)
    return (row * side + column) * 2 + core


def first_groups(side):
    return [
        [flat_index(first, second, core, side) for first in range(side)]
        for core in range(2)
        for second in range(side)
    ]


def shifted(value, shift, side):
    moves = []
    for core in range(2):
        for first in range(side):
            for second in range(side):
                target = (second + shift) % side
                moves.append(
                    (flat_index(first, second, core, side), flat_index(first, target, core, side))
                )
    return lax.ppermute(value, pair, moves)


def swapped(value, axis):
    return lax.ppermute(value, axis, [(0, 1), (1, 0)])


def on_chip(kernel, out_shapes, operands, scratch=(), limit=16):
    return pl.pallas_call(
        kernel,
        out_shape=out_shapes,
        in_specs=[
            pl.BlockSpec(memory_space=pltpu.SMEM if a.ndim == 1 else pltpu.VMEM) for a in operands
        ],
        out_specs=jax.tree.map(lambda _: pl.BlockSpec(memory_space=pltpu.VMEM), out_shapes),
        scratch_shapes=list(scratch),
        compiler_params=pltpu.CompilerParams(vmem_limit_bytes=limit * 1024 * 1024),
    )(*operands)


def message_kernel(place_ref, hidden_ref, own_ref, other_ref, mask_ref, message_ref, sum_ref):
    side, _, width = message_ref.shape
    half = hidden_ref.shape[1]
    lanes = width - half
    expert_count = mask_ref.shape[1]
    core, second = place_ref[1], place_ref[2]
    chosen = jnp.where(mask_ref[...] > 0, jax.nn.sigmoid(own_ref[...] + other_ref[...]), 0.0)
    affinity_sum = jnp.sum(chosen, axis=1, keepdims=True)
    sum_ref[...] = affinity_sum
    gates = jnp.where(affinity_sum > 0, routed_scale * chosen / affinity_sum, 0.0)
    parts = jnp.concatenate([part.astype(jnp.float32) for part in split_in_two(gates)], axis=1)
    shape = (2 * expert_count, side * lanes)
    source = lax.broadcasted_iota(jnp.int32, shape, 0)
    column = lax.broadcasted_iota(jnp.int32, shape, 1)
    first = lax.div(column, lanes)
    lane = column - first * lanes
    low = (lane >= side).astype(jnp.int32)
    ahead = lax.rem(lane - low * side + second, side)
    wanted = jnp.where(core == 0, ahead * side + first, first * side + ahead) + low * expert_count
    select = jnp.where((lane < 2 * side) & (wanted == source), 1.0, 0.0).astype(jnp.bfloat16)
    picked = jnp.dot(parts.astype(jnp.bfloat16), select, preferred_element_type=jnp.float32)
    picked = picked.astype(jnp.bfloat16)
    for first in range(side):
        message_ref[first, :, pl.ds(0, half)] = hidden_ref[...]
        message_ref[first, :, pl.ds(half, lanes)] = picked[:, first * lanes : (first + 1) * lanes]


def fetch_kernel(side, *refs):
    sources, (slot_ref, gate_ref, _), refs = refs[:3], refs[3:6], refs[6:]
    targets, taking, sems = refs[:3], refs[3], refs[4:]
    copies = [pltpu.make_async_copy(s, t, m) for s, t, m in zip(sources, targets, sems)]
    for copy in copies:
        copy.start()
    line_tokens = slot_ref.shape[0]
    slots = taking.shape[1] // side
    slot_iota = lax.broadcasted_iota(jnp.int32, (line_tokens, slots), 1)
    steps = far_to_near(side)
    for place in range(0, side, 2):
        columns = pl.ds(place * slots, 2 * slots)
        pair_of = steps[place : place + 2]
        for index in range(2):
            taken = [
                jnp.where(
                    slot_ref[:, s : s + 1] == slot_iota,
                    gate_ref[:, index * side + s : index * side + s + 1],
                    0.0,
                )
                for s in pair_of
            ]
            taking[pl.ds(index * line_tokens, line_tokens), columns] = jnp.concatenate(
                taken, axis=1
            ).astype(jnp.bfloat16)
    for copy in copies:
        copy.wait()


def fetched(arrays, side, slot, gates, after):
    line_tokens = slot.shape[0]
    taking_shape = (2 * line_tokens, side * after.shape[0])
    vmem = pl.BlockSpec(memory_space=pltpu.VMEM)
    return pl.pallas_call(
        lambda *refs: fetch_kernel(side, *refs),
        out_shape=tuple(pltpu.VMEM(a.shape, a.dtype) for a in arrays)
        + (jax.ShapeDtypeStruct(taking_shape, jnp.bfloat16),),
        in_specs=[pl.BlockSpec(memory_space=pltpu.HBM)] * 3
        + [vmem] * 2
        + [pl.BlockSpec(memory_space=pl.ANY)],
        out_specs=(vmem,) * 4,
        scratch_shapes=[pltpu.SemaphoreType.DMA] * len(arrays),
        compiler_params=pltpu.CompilerParams(vmem_limit_bytes=42 * 1024 * 1024),
        name="fetch_weights",
    )(*arrays, slot, gates, after)


def select_kernel(capacity, place_ref, line_ref, *refs):
    part_refs, (slot_ref, gate_ref) = refs[:-2], refs[-2:]
    side, token_count, width = line_ref.shape
    slots, half = part_refs[0].shape
    line_tokens = side * token_count
    first = place_ref[3]
    gates = line_ref[:, :, pl.ds(half, width - half)].reshape(line_tokens, width - half)
    gates = gates.astype(jnp.float32)
    gate_ref[...] = gates
    shape = (line_tokens, line_tokens)
    later = lax.broadcasted_iota(jnp.int32, shape, 0)
    earlier = lax.broadcasted_iota(jnp.int32, shape, 1)
    same = lax.div(later, token_count) == lax.div(earlier, token_count)
    before = jnp.where(same & (later > earlier), 1.0, 0.0).astype(jnp.bfloat16)
    picked = jnp.where(gates != 0, 1.0, 0.0).astype(jnp.bfloat16)
    rank = jnp.dot(before, picked, preferred_element_type=jnp.float32)
    block = lax.div(lax.broadcasted_iota(jnp.int32, gates.shape, 0), token_count)
    offset = lax.rem(first - block + side, side) * capacity
    slot = jnp.where(gates != 0, offset.astype(jnp.float32) + rank, -1.0)
    slot_ref[...] = slot.astype(jnp.int32)
    slot_rows = jnp.transpose(slot).astype(jnp.int32)
    tokens = line_ref[:, :, pl.ds(0, half)].reshape(line_tokens, half)
    slot_iota = lax.broadcasted_iota(jnp.int32, (slots, line_tokens), 0)
    for step in range(side):
        placing = jnp.where(slot_rows[step : step + 1, :] == slot_iota, 1.0, 0.0)
        rows = jnp.dot(placing.astype(jnp.bfloat16), tokens, preferred_element_type=jnp.float32)
        part_refs[step][...] = rows.astype(jnp.bfloat16)


def far_to_near(side):
    return sorted(range(side), key=lambda step: (-min(step, side - step), step))


def by_step(parts):
    steps = far_to_near(len(parts))
    return [parts[steps.index(step)] for step in range(len(parts))]


def expert_kernel(side, start_ref, gate_ref, up_ref, down_ref, *refs):
    own_refs, other_refs = by_step(refs[:side]), by_step(refs[side : 2 * side])
    active_ref, sent_ref, own, other = refs[2 * side :]
    early = early_parts(side)
    slots, half = own_refs[0].shape
    capacity = slots // side
    width = gate_ref.shape[1]
    for step in range(side):
        rows = pl.ds(step * slots, slots)
        own[rows, :] = own_refs[step][...]
        for block in range(side):
            other[pl.ds(step * slots + block * capacity, capacity), :] = other_refs[block][
                pl.ds(step * capacity, capacity), :
            ]
    mine = pl.multiple_of(start_ref[0], 256)
    theirs = pl.multiple_of(half - mine, 256)

    def product(weight_ref, columns):
        return jnp.dot(
            own[...], weight_ref[pl.ds(mine, half), columns], preferred_element_type=jnp.float32
        ) + jnp.dot(
            other[...], weight_ref[pl.ds(theirs, half), columns], preferred_element_type=jnp.float32
        )

    tile = 256
    for column in range(0, width, tile):
        columns = pl.ds(column, tile)
        gate_part = product(gate_ref, columns)
        up_part = product(up_ref, columns)
        active_ref[:, columns] = (jax.nn.silu(gate_part) * up_part).astype(jnp.bfloat16)
    send_blocks(early, theirs, active_ref, down_ref, sent_ref)


def early_parts(side):
    return far_to_near(side)[: side // 2 - 1]


def late_parts(side):
    return far_to_near(side)[side // 2 - 1 :]


def send_blocks(blocks, theirs, active_ref, down_ref, sent_ref):
    count, slots, half = sent_ref.shape
    width = active_ref.shape[1]
    side = active_ref.shape[0] // slots
    capacity = slots // side
    active = active_ref[...].reshape(side, side, capacity, width)
    rows = jnp.concatenate([active[:, block].reshape(slots, width) for block in blocks], axis=0)
    tile = 256
    for column in range(0, half, tile):
        weight = down_ref[:, pl.ds(pl.multiple_of(theirs + column, 256), tile)]
        sent = jnp.dot(rows, weight, preferred_element_type=jnp.float32).astype(jnp.bfloat16)
        sent_ref[:, :, pl.ds(column, tile)] = sent.reshape(count, slots, tile)


def late_kernel(side, start_ref, active_ref, down_ref, sent_ref):
    theirs = pl.multiple_of(sent_ref.shape[2] - start_ref[0], 256)
    send_blocks(late_parts(side), theirs, active_ref, down_ref, sent_ref)


def finish_kernel(steps, start_ref, active_ref, down_ref, arrived_ref, *part_refs):
    slots, half = part_refs[0].shape
    mine = start_ref[0]
    rows = jnp.concatenate([active_ref[pl.ds(step * slots, slots), :] for step in steps], axis=0)
    tile = 256
    for column in range(0, half, tile):
        columns = pl.ds(column, tile)
        weight = down_ref[:, pl.ds(pl.multiple_of(mine + column, 256), tile)]
        kept = jnp.dot(rows, weight, preferred_element_type=jnp.float32)
        for index in range(len(steps)):
            arrived = arrived_ref[index, :, columns].astype(jnp.float32)
            part_refs[index][:, columns] = (
                kept[index * slots : (index + 1) * slots] + arrived
            ).astype(jnp.bfloat16)


def gather_kernel(place, taking_ref, *refs):
    back_refs, (out_ref, rows) = refs[:-2], refs[-2:]
    slots, half = back_refs[0].shape
    depth = len(back_refs) * slots
    for index, back_ref in enumerate(back_refs):
        rows[pl.ds(index * slots, slots), :] = back_ref[...]
    taking = taking_ref[:, place * slots : place * slots + depth]
    line_tokens = taking.shape[0] // 2
    tile = 256
    for column in range(0, half, tile):
        columns = pl.ds(column, tile)
        both = jnp.dot(taking, rows[:, columns], preferred_element_type=jnp.float32)
        out_ref[:, columns] = both[:line_tokens] + both[line_tokens:]


def combine_kernel(place, taking_ref, sofar_ref, *refs):
    back_refs, (out_ref, rows) = refs[:-2], refs[-2:]
    slots, half = back_refs[0].shape
    depth = len(back_refs) * slots
    for index, back_ref in enumerate(back_refs):
        rows[pl.ds(index * slots, slots), :] = back_ref[...]
    taking = taking_ref[:, place * slots : place * slots + depth]
    line_tokens = taking.shape[0] // 2
    tile = 256
    for column in range(0, half, tile):
        columns = pl.ds(column, tile)
        both = jnp.dot(taking, rows[:, columns], preferred_element_type=jnp.float32)
        total = sofar_ref[:, columns] + both[:line_tokens] + both[line_tokens:]
        out_ref[:, :, columns] = total.astype(jnp.bfloat16).reshape(
            out_ref.shape[0], out_ref.shape[1], tile
        )


def total_kernel(sum_ref, share_ref, out_ref):
    total = share_ref[0].astype(jnp.float32)
    for step in range(1, share_ref.shape[0]):
        total = total + share_ref[step].astype(jnp.float32)
    out_ref[...] = jnp.where(sum_ref[...] > 0, total, jnp.nan).astype(out_ref.dtype)


def split_in_two(value):
    high = value.astype(jnp.bfloat16)
    return high, (value - high.astype(jnp.float32)).astype(jnp.bfloat16)


def attention_kernel(lengths_ref, q_latent_ref, q_rope_ref, latent_ref, rope_ref, out_ref):
    for sequence in range(q_latent_ref.shape[0]):
        latent = latent_ref[sequence]
        scores = lax.dot_general(
            q_latent_ref[sequence], latent, (((1,), (1,)), ((), ())), preferred_element_type=jnp.float32
        ) + jnp.dot(q_rope_ref[sequence], rope_ref[sequence], preferred_element_type=jnp.float32)
        position = lax.broadcasted_iota(jnp.int32, scores.shape, 1)
        live = position < lengths_ref[sequence]
        scores = jnp.where(live, scores * softmax_scale, -jnp.inf)
        highest = jnp.max(scores, axis=1, keepdims=True)
        expo = jnp.where(live, jnp.exp(scores - highest), 0.0)
        probs = (expo / jnp.sum(expo, axis=1, keepdims=True)).astype(jnp.bfloat16)
        mixed = jnp.dot(probs, latent, preferred_element_type=jnp.float32)
        out_ref[sequence] = mixed.astype(jnp.bfloat16)


def local(
    hidden,
    routes,
    router_weight,
    gate_weight,
    up_weight,
    down_weight,
    q_latent,
    q_rope,
    cache_latent,
    cache_rope,
    lengths,
):
    token_count, top_count = routes.shape
    expert_count = lax.axis_size("ep")
    side = side_of(expert_count)
    capacity = min(token_count, 4 * token_count * top_count // expert_count)
    line_slots = side * capacity
    line_tokens = side * token_count
    half = hidden.shape[1]
    bf16, f32 = jnp.bfloat16, jnp.float32

    core = lax.axis_index("tp")
    place = lax.axis_index("ep")
    row, column = place // side, place % side
    first = jnp.where(core == 0, column, row)
    second = jnp.where(core == 0, row, column)
    start = jnp.stack([core * half, core, second, first]).astype(jnp.int32)

    expert_iota = jnp.arange(expert_count, dtype=jnp.int32)
    mask = jnp.sum((routes.T[:, :, None] == expert_iota).astype(f32), axis=0)
    partial_logits = jnp.dot(hidden, router_weight, preferred_element_type=f32)
    other_logits = swapped(partial_logits, "tp")

    lanes = 128 * ((2 * side + 127) // 128)
    message, affinity_sum = on_chip(
        message_kernel,
        (
            jax.ShapeDtypeStruct((side, token_count, half + lanes), bf16),
            jax.ShapeDtypeStruct((token_count, 1), f32),
        ),
        (start, hidden, partial_logits, other_logits, mask),
    )
    line = lax.all_to_all(
        message, pair, 0, 0, axis_index_groups=first_groups(side), tiled=True
    )
    part_shape = jax.ShapeDtypeStruct((line_slots, half), bf16)
    *rows, slot, line_gates = on_chip(
        lambda *refs: select_kernel(capacity, *refs),
        (part_shape,) * side
        + (
            jax.ShapeDtypeStruct((line_tokens, lanes), jnp.int32),
            jax.ShapeDtypeStruct((line_tokens, lanes), f32),
        ),
        (start, line),
    )

    order = [step for step in far_to_near(side) if step]
    own, other = [rows[0]] + [None] * (side - 1), [None] * side
    for step in order:
        own[step] = shifted(rows[step], step, side)
    weights = (gate_weight[0], up_weight[0], down_weight[0])
    *weights, taking = fetched(weights, side, slot, line_gates, rows[0])
    other[0] = swapped(own[0], "tp")
    own[order[0]], *weights = lax.optimization_barrier((own[order[0]], *weights))
    for step in order:
        other[step] = swapped(own[step], "tp")
    gate_w, up_w, down_w = weights

    attn_latent = on_chip(
        attention_kernel,
        jax.ShapeDtypeStruct(q_latent.shape, bf16),
        (lengths, q_latent, q_rope, cache_latent, cache_rope),
    )

    all_slots = side * line_slots
    rows_scratch = pltpu.VMEM((all_slots, half), bf16)
    early, late = early_parts(side), late_parts(side)
    steps = far_to_near(side)
    active, sent = on_chip(
        lambda *refs: expert_kernel(side, *refs),
        (
            jax.ShapeDtypeStruct((all_slots, gate_w.shape[1]), bf16),
            jax.ShapeDtypeStruct((len(early), line_slots, half), bf16),
        ),
        (start, gate_w, up_w, down_w, *(own[s] for s in steps), *(other[s] for s in steps)),
        (rows_scratch, rows_scratch),
        16,
    )
    early_arrived = swapped(sent, "tp")
    late_sent = on_chip(
        lambda *refs: late_kernel(side, *refs),
        jax.ShapeDtypeStruct((len(late), line_slots, half), bf16),
        (start, active, down_w),
    )
    late_arrived = swapped(late_sent, "tp")
    summed = {}
    for steps_of, arrived in ((early, early_arrived), (late, late_arrived)):
        parts = on_chip(
            lambda *refs, steps_of=steps_of: finish_kernel(steps_of, *refs),
            (part_shape,) * len(steps_of),
            (start, active, down_w, arrived),
        )
        summed.update(zip(steps_of, parts))

    back = {0: summed[0]}
    for step in order[:-1]:
        back[step] = shifted(summed[step], -step, side)
    back[order[-1]] = shifted(summed[order[-1]], -order[-1], side)
    cut = side // 2
    half_scratch = pltpu.VMEM((cut * line_slots, half), bf16)
    sofar = on_chip(
        lambda *refs: gather_kernel(0, *refs),
        jax.ShapeDtypeStruct((line_tokens, half), f32),
        (taking, *(back[s] for s in steps[:cut])),
        (half_scratch,),
    )
    weighted = on_chip(
        lambda *refs: combine_kernel(cut, *refs),
        jax.ShapeDtypeStruct((side, token_count, half), bf16),
        (taking, sofar, *(back[s] for s in steps[cut:])),
        (half_scratch,),
    )
    shares = lax.all_to_all(
        weighted, pair, 0, 0, axis_index_groups=first_groups(side), tiled=True
    )
    moe_out = on_chip(
        total_kernel, jax.ShapeDtypeStruct((token_count, half), bf16), (affinity_sum, shares)
    )
    return (moe_out, attn_latent)


def solution(mesh):
    return jax.shard_map(
        local,
        mesh=mesh,
        in_specs=(
            P(("groups", "ep"), "tp"),
            P(("groups", "ep"), None),
            P("tp", None),
            P("ep", None, "tp"),
            P("ep", None, "tp"),
            P("ep", "tp", None),
            P(("groups", "ep"), "tp", None),
            P(("groups", "ep"), "tp", None),
            P(("groups", "ep"), None, None),
            P(("groups", "ep"), None, None),
            P(("groups", "ep")),
        ),
        out_specs=(P(("groups", "ep"), "tp"), P(("groups", "ep"), "tp", None)),
        check_vma=False,
    )
```

```python
import math

import jax
import jax.numpy as jnp
from jax import lax
from jax.experimental import pallas as pl
from jax.experimental.pallas import tpu as pltpu
from jax.sharding import PartitionSpec as P


softmax_scale = 192.0 ** (-0.5)
routed_scale = 2.5
pair = ("ep", "tp")


def side_of(devices):
    side = math.isqrt(devices)
    assert side * side == devices
    return side


def flat_index(first, second, core, side):
    row, column = (second, first) if core == 0 else (first, second)
    return (row * side + column) * 2 + core


def first_groups(side):
    return [
        [flat_index(first, second, core, side) for first in range(side)]
        for core in range(2)
        for second in range(side)
    ]


def shifted(value, shift, side):
    moves = []
    for core in range(2):
        for first in range(side):
            for second in range(side):
                target = (second + shift) % side
                moves.append(
                    (flat_index(first, second, core, side), flat_index(first, target, core, side))
                )
    return lax.ppermute(value, pair, moves)


def swapped(value, axis):
    return lax.ppermute(value, axis, [(0, 1), (1, 0)])


def on_chip(kernel, out_shapes, operands, scratch=(), limit=16):
    return pl.pallas_call(
        kernel,
        out_shape=out_shapes,
        in_specs=[
            pl.BlockSpec(memory_space=pltpu.SMEM if a.ndim == 1 else pltpu.VMEM) for a in operands
        ],
        out_specs=jax.tree.map(lambda _: pl.BlockSpec(memory_space=pltpu.VMEM), out_shapes),
        scratch_shapes=list(scratch),
        compiler_params=pltpu.CompilerParams(vmem_limit_bytes=limit * 1024 * 1024),
    )(*operands)


def router_kernel(hidden_ref, weight_ref, logits_ref, tokens_ref, weight, sems):
    copies = [
        pltpu.make_async_copy(hidden_ref, tokens_ref, sems.at[0]),
        pltpu.make_async_copy(weight_ref, weight, sems.at[1]),
    ]
    for copy in copies:
        copy.start()
    for copy in copies:
        copy.wait()
    logits_ref[...] = lax.dot_general(
        tokens_ref[...], weight[...], (((1,), (1,)), ((), ())), preferred_element_type=jnp.float32
    )


def routed(hidden, weight):
    vmem = pl.BlockSpec(memory_space=pltpu.VMEM)
    return pl.pallas_call(
        router_kernel,
        out_shape=(
            pltpu.VMEM((hidden.shape[0], weight.shape[0]), jnp.float32),
            pltpu.VMEM(hidden.shape, hidden.dtype),
        ),
        in_specs=[pl.BlockSpec(memory_space=pltpu.HBM)] * 2,
        out_specs=(vmem, vmem),
        scratch_shapes=[
            pltpu.VMEM(weight.shape, weight.dtype),
            pltpu.SemaphoreType.DMA((2,)),
        ],
        compiler_params=pltpu.CompilerParams(vmem_limit_bytes=63 * 1024 * 1024 + 512 * 1024),
        name="router",
    )(hidden, weight)


def message_kernel(place_ref, hidden_ref, own_ref, other_ref, mask_ref, message_ref, sum_ref):
    side, _, width = message_ref.shape
    half = hidden_ref.shape[1]
    lanes = width - half
    expert_count = mask_ref.shape[1]
    core, second = place_ref[1], place_ref[2]
    chosen = jnp.where(mask_ref[...] > 0, jax.nn.sigmoid(own_ref[...] + other_ref[...]), 0.0)
    affinity_sum = jnp.sum(chosen, axis=1, keepdims=True)
    sum_ref[...] = affinity_sum
    gates = jnp.where(affinity_sum > 0, routed_scale * chosen / affinity_sum, 0.0)
    parts = jnp.concatenate([part.astype(jnp.float32) for part in split_in_two(gates)], axis=1)
    shape = (2 * expert_count, side * lanes)
    source = lax.broadcasted_iota(jnp.int32, shape, 0)
    column = lax.broadcasted_iota(jnp.int32, shape, 1)
    first = lax.div(column, lanes)
    lane = column - first * lanes
    low = (lane >= side).astype(jnp.int32)
    ahead = lax.rem(lane - low * side + second, side)
    wanted = jnp.where(core == 0, ahead * side + first, first * side + ahead) + low * expert_count
    select = jnp.where((lane < 2 * side) & (wanted == source), 1.0, 0.0).astype(jnp.bfloat16)
    picked = jnp.dot(parts.astype(jnp.bfloat16), select, preferred_element_type=jnp.float32)
    picked = picked.astype(jnp.bfloat16)
    for first in range(side):
        message_ref[first, :, pl.ds(0, half)] = hidden_ref[...]
        message_ref[first, :, pl.ds(half, lanes)] = picked[:, first * lanes : (first + 1) * lanes]


def fetch_kernel(side, *refs):
    sources, (slot_ref, gate_ref, _), refs = refs[:3], refs[3:6], refs[6:]
    targets, taking, sems = refs[:3], refs[3], refs[4:]
    copies = [pltpu.make_async_copy(s, t, m) for s, t, m in zip(sources, targets, sems)]
    for copy in copies:
        copy.start()
    line_tokens = slot_ref.shape[0]
    slots = taking.shape[1] // side
    slot_iota = lax.broadcasted_iota(jnp.int32, (line_tokens, slots), 1)
    steps = far_to_near(side)
    for place in range(0, side, 2):
        columns = pl.ds(place * slots, 2 * slots)
        pair_of = steps[place : place + 2]
        for index in range(2):
            taken = [
                jnp.where(
                    slot_ref[:, s : s + 1] == slot_iota,
                    gate_ref[:, index * side + s : index * side + s + 1],
                    0.0,
                )
                for s in pair_of
            ]
            taking[pl.ds(index * line_tokens, line_tokens), columns] = jnp.concatenate(
                taken, axis=1
            ).astype(jnp.bfloat16)
    for copy in copies:
        copy.wait()


def fetched(arrays, side, slot, gates, after):
    line_tokens = slot.shape[0]
    taking_shape = (2 * line_tokens, side * after.shape[0])
    vmem = pl.BlockSpec(memory_space=pltpu.VMEM)
    return pl.pallas_call(
        lambda *refs: fetch_kernel(side, *refs),
        out_shape=tuple(pltpu.VMEM(a.shape, a.dtype) for a in arrays)
        + (jax.ShapeDtypeStruct(taking_shape, jnp.bfloat16),),
        in_specs=[pl.BlockSpec(memory_space=pltpu.HBM)] * 3
        + [vmem] * 2
        + [pl.BlockSpec(memory_space=pl.ANY)],
        out_specs=(vmem,) * 4,
        scratch_shapes=[pltpu.SemaphoreType.DMA] * len(arrays),
        compiler_params=pltpu.CompilerParams(vmem_limit_bytes=42 * 1024 * 1024),
        name="fetch_weights",
    )(*arrays, slot, gates, after)


def select_kernel(capacity, place_ref, line_ref, *refs):
    part_refs, (slot_ref, gate_ref) = refs[:-2], refs[-2:]
    side, token_count, width = line_ref.shape
    slots, half = part_refs[0].shape
    line_tokens = side * token_count
    first = place_ref[3]
    gates = line_ref[:, :, pl.ds(half, width - half)].reshape(line_tokens, width - half)
    gates = gates.astype(jnp.float32)
    gate_ref[...] = gates
    shape = (line_tokens, line_tokens)
    later = lax.broadcasted_iota(jnp.int32, shape, 0)
    earlier = lax.broadcasted_iota(jnp.int32, shape, 1)
    same = lax.div(later, token_count) == lax.div(earlier, token_count)
    before = jnp.where(same & (later > earlier), 1.0, 0.0).astype(jnp.bfloat16)
    picked = jnp.where(gates != 0, 1.0, 0.0).astype(jnp.bfloat16)
    rank = jnp.dot(before, picked, preferred_element_type=jnp.float32)
    block = lax.div(lax.broadcasted_iota(jnp.int32, gates.shape, 0), token_count)
    offset = lax.rem(first - block + side, side) * capacity
    slot = jnp.where(gates != 0, offset.astype(jnp.float32) + rank, -1.0)
    slot_ref[...] = slot.astype(jnp.int32)
    slot_rows = jnp.transpose(slot).astype(jnp.int32)
    tokens = line_ref[:, :, pl.ds(0, half)].reshape(line_tokens, half)
    slot_iota = lax.broadcasted_iota(jnp.int32, (slots, line_tokens), 0)
    for step in range(side):
        placing = jnp.where(slot_rows[step : step + 1, :] == slot_iota, 1.0, 0.0)
        rows = jnp.dot(placing.astype(jnp.bfloat16), tokens, preferred_element_type=jnp.float32)
        part_refs[step][...] = rows.astype(jnp.bfloat16)


def far_to_near(side):
    return sorted(range(side), key=lambda step: (-min(step, side - step), step))


def by_step(parts):
    steps = far_to_near(len(parts))
    return [parts[steps.index(step)] for step in range(len(parts))]


def expert_kernel(side, start_ref, gate_ref, up_ref, down_ref, *refs):
    own_refs, other_refs = by_step(refs[:side]), by_step(refs[side : 2 * side])
    active_ref, sent_ref, own, other = refs[2 * side :]
    early = early_parts(side)
    slots, half = own_refs[0].shape
    capacity = slots // side
    width = gate_ref.shape[1]
    for step in range(side):
        rows = pl.ds(step * slots, slots)
        own[rows, :] = own_refs[step][...]
        for block in range(side):
            other[pl.ds(step * slots + block * capacity, capacity), :] = other_refs[block][
                pl.ds(step * capacity, capacity), :
            ]
    mine = pl.multiple_of(start_ref[0], 256)
    theirs = pl.multiple_of(half - mine, 256)

    def product(weight_ref, columns):
        return jnp.dot(
            own[...], weight_ref[pl.ds(mine, half), columns], preferred_element_type=jnp.float32
        ) + jnp.dot(
            other[...], weight_ref[pl.ds(theirs, half), columns], preferred_element_type=jnp.float32
        )

    tile = 256
    for column in range(0, width, tile):
        columns = pl.ds(column, tile)
        gate_part = product(gate_ref, columns)
        up_part = product(up_ref, columns)
        active_ref[:, columns] = (jax.nn.silu(gate_part) * up_part).astype(jnp.bfloat16)
    send_blocks(early, theirs, active_ref, down_ref, sent_ref)


def early_parts(side):
    return far_to_near(side)[: side // 2 - 1]


def late_parts(side):
    return far_to_near(side)[side // 2 - 1 :]


def send_blocks(blocks, theirs, active_ref, down_ref, sent_ref):
    count, slots, half = sent_ref.shape
    width = active_ref.shape[1]
    side = active_ref.shape[0] // slots
    capacity = slots // side
    active = active_ref[...].reshape(side, side, capacity, width)
    rows = jnp.concatenate([active[:, block].reshape(slots, width) for block in blocks], axis=0)
    tile = 256
    for column in range(0, half, tile):
        weight = down_ref[:, pl.ds(pl.multiple_of(theirs + column, 256), tile)]
        sent = jnp.dot(rows, weight, preferred_element_type=jnp.float32).astype(jnp.bfloat16)
        sent_ref[:, :, pl.ds(column, tile)] = sent.reshape(count, slots, tile)


def late_kernel(side, start_ref, active_ref, down_ref, sent_ref):
    theirs = pl.multiple_of(sent_ref.shape[2] - start_ref[0], 256)
    send_blocks(late_parts(side), theirs, active_ref, down_ref, sent_ref)


def finish_kernel(steps, start_ref, active_ref, down_ref, arrived_ref, *part_refs):
    slots, half = part_refs[0].shape
    mine = start_ref[0]
    rows = jnp.concatenate([active_ref[pl.ds(step * slots, slots), :] for step in steps], axis=0)
    tile = 256
    for column in range(0, half, tile):
        columns = pl.ds(column, tile)
        weight = down_ref[:, pl.ds(pl.multiple_of(mine + column, 256), tile)]
        kept = jnp.dot(rows, weight, preferred_element_type=jnp.float32)
        for index in range(len(steps)):
            arrived = arrived_ref[index, :, columns].astype(jnp.float32)
            part_refs[index][:, columns] = (
                kept[index * slots : (index + 1) * slots] + arrived
            ).astype(jnp.bfloat16)


def gather_kernel(place, taking_ref, *refs):
    back_refs, (out_ref, rows) = refs[:-2], refs[-2:]
    slots, half = back_refs[0].shape
    depth = len(back_refs) * slots
    for index, back_ref in enumerate(back_refs):
        rows[pl.ds(index * slots, slots), :] = back_ref[...]
    taking = taking_ref[:, place * slots : place * slots + depth]
    line_tokens = taking.shape[0] // 2
    tile = 256
    for column in range(0, half, tile):
        columns = pl.ds(column, tile)
        both = jnp.dot(taking, rows[:, columns], preferred_element_type=jnp.float32)
        out_ref[:, columns] = both[:line_tokens] + both[line_tokens:]


def combine_kernel(place, taking_ref, sofar_ref, *refs):
    back_refs, (out_ref, rows) = refs[:-2], refs[-2:]
    slots, half = back_refs[0].shape
    depth = len(back_refs) * slots
    for index, back_ref in enumerate(back_refs):
        rows[pl.ds(index * slots, slots), :] = back_ref[...]
    taking = taking_ref[:, place * slots : place * slots + depth]
    line_tokens = taking.shape[0] // 2
    tile = 256
    for column in range(0, half, tile):
        columns = pl.ds(column, tile)
        both = jnp.dot(taking, rows[:, columns], preferred_element_type=jnp.float32)
        total = sofar_ref[:, columns] + both[:line_tokens] + both[line_tokens:]
        out_ref[:, :, columns] = total.astype(jnp.bfloat16).reshape(
            out_ref.shape[0], out_ref.shape[1], tile
        )


def total_kernel(sum_ref, share_ref, out_ref):
    total = share_ref[0].astype(jnp.float32)
    for step in range(1, share_ref.shape[0]):
        total = total + share_ref[step].astype(jnp.float32)
    out_ref[...] = jnp.where(sum_ref[...] > 0, total, jnp.nan).astype(out_ref.dtype)


def split_in_two(value):
    high = value.astype(jnp.bfloat16)
    return high, (value - high.astype(jnp.float32)).astype(jnp.bfloat16)


def attention_kernel(lengths_ref, q_latent_ref, q_rope_ref, latent_ref, rope_ref, out_ref):
    for sequence in range(q_latent_ref.shape[0]):
        latent = latent_ref[sequence]
        scores = lax.dot_general(
            q_latent_ref[sequence], latent, (((1,), (1,)), ((), ())), preferred_element_type=jnp.float32
        ) + jnp.dot(q_rope_ref[sequence], rope_ref[sequence], preferred_element_type=jnp.float32)
        position = lax.broadcasted_iota(jnp.int32, scores.shape, 1)
        live = position < lengths_ref[sequence]
        scores = jnp.where(live, scores * softmax_scale, -jnp.inf)
        highest = jnp.max(scores, axis=1, keepdims=True)
        expo = jnp.where(live, jnp.exp(scores - highest), 0.0)
        probs = (expo / jnp.sum(expo, axis=1, keepdims=True)).astype(jnp.bfloat16)
        mixed = jnp.dot(probs, latent, preferred_element_type=jnp.float32)
        out_ref[sequence] = mixed.astype(jnp.bfloat16)


def local(
    hidden,
    routes,
    router_weight,
    gate_weight,
    up_weight,
    down_weight,
    q_latent,
    q_rope,
    cache_latent,
    cache_rope,
    lengths,
):
    token_count, top_count = routes.shape
    expert_count = lax.axis_size("ep")
    side = side_of(expert_count)
    capacity = min(token_count, 4 * token_count * top_count // expert_count)
    line_slots = side * capacity
    line_tokens = side * token_count
    half = hidden.shape[1]
    bf16, f32 = jnp.bfloat16, jnp.float32

    core = lax.axis_index("tp")
    place = lax.axis_index("ep")
    row, column = place // side, place % side
    first = jnp.where(core == 0, column, row)
    second = jnp.where(core == 0, row, column)
    start = jnp.stack([core * half, core, second, first]).astype(jnp.int32)

    expert_iota = jnp.arange(expert_count, dtype=jnp.int32)
    mask = jnp.sum((routes.T[:, :, None] == expert_iota).astype(f32), axis=0)
    partial_logits, hidden = routed(hidden, router_weight.T)
    other_logits = swapped(partial_logits, "tp")

    lanes = 128 * ((2 * side + 127) // 128)
    message, affinity_sum = on_chip(
        message_kernel,
        (
            jax.ShapeDtypeStruct((side, token_count, half + lanes), bf16),
            jax.ShapeDtypeStruct((token_count, 1), f32),
        ),
        (start, hidden, partial_logits, other_logits, mask),
    )
    line = lax.all_to_all(
        message, pair, 0, 0, axis_index_groups=first_groups(side), tiled=True
    )
    part_shape = jax.ShapeDtypeStruct((line_slots, half), bf16)
    *rows, slot, line_gates = on_chip(
        lambda *refs: select_kernel(capacity, *refs),
        (part_shape,) * side
        + (
            jax.ShapeDtypeStruct((line_tokens, lanes), jnp.int32),
            jax.ShapeDtypeStruct((line_tokens, lanes), f32),
        ),
        (start, line),
    )

    order = [step for step in far_to_near(side) if step]
    own, other = [rows[0]] + [None] * (side - 1), [None] * side
    for step in order:
        own[step] = shifted(rows[step], step, side)
    weights = (gate_weight[0], up_weight[0], down_weight[0])
    *weights, taking = fetched(weights, side, slot, line_gates, rows[0])
    other[0] = swapped(own[0], "tp")
    own[order[0]], *weights = lax.optimization_barrier((own[order[0]], *weights))
    for step in order:
        other[step] = swapped(own[step], "tp")
    gate_w, up_w, down_w = weights

    attn_latent = on_chip(
        attention_kernel,
        jax.ShapeDtypeStruct(q_latent.shape, bf16),
        (lengths, q_latent, q_rope, cache_latent, cache_rope),
    )

    all_slots = side * line_slots
    rows_scratch = pltpu.VMEM((all_slots, half), bf16)
    early, late = early_parts(side), late_parts(side)
    steps = far_to_near(side)
    active, sent = on_chip(
        lambda *refs: expert_kernel(side, *refs),
        (
            jax.ShapeDtypeStruct((all_slots, gate_w.shape[1]), bf16),
            jax.ShapeDtypeStruct((len(early), line_slots, half), bf16),
        ),
        (start, gate_w, up_w, down_w, *(own[s] for s in steps), *(other[s] for s in steps)),
        (rows_scratch, rows_scratch),
        16,
    )
    early_arrived = swapped(sent, "tp")
    late_sent = on_chip(
        lambda *refs: late_kernel(side, *refs),
        jax.ShapeDtypeStruct((len(late), line_slots, half), bf16),
        (start, active, down_w),
    )
    late_arrived = swapped(late_sent, "tp")
    summed = {}
    for steps_of, arrived in ((early, early_arrived), (late, late_arrived)):
        parts = on_chip(
            lambda *refs, steps_of=steps_of: finish_kernel(steps_of, *refs),
            (part_shape,) * len(steps_of),
            (start, active, down_w, arrived),
        )
        summed.update(zip(steps_of, parts))

    back = {0: summed[0]}
    for step in order[:-1]:
        back[step] = shifted(summed[step], -step, side)
    back[order[-1]] = shifted(summed[order[-1]], -order[-1], side)
    cut = side // 2
    half_scratch = pltpu.VMEM((cut * line_slots, half), bf16)
    sofar = on_chip(
        lambda *refs: gather_kernel(0, *refs),
        jax.ShapeDtypeStruct((line_tokens, half), f32),
        (taking, *(back[s] for s in steps[:cut])),
        (half_scratch,),
    )
    weighted = on_chip(
        lambda *refs: combine_kernel(cut, *refs),
        jax.ShapeDtypeStruct((side, token_count, half), bf16),
        (taking, sofar, *(back[s] for s in steps[cut:])),
        (half_scratch,),
    )
    shares = lax.all_to_all(
        weighted, pair, 0, 0, axis_index_groups=first_groups(side), tiled=True
    )
    moe_out = on_chip(
        total_kernel, jax.ShapeDtypeStruct((token_count, half), bf16), (affinity_sum, shares)
    )
    return (moe_out, attn_latent)


def solution(mesh):
    return jax.shard_map(
        local,
        mesh=mesh,
        in_specs=(
            P(("groups", "ep"), "tp"),
            P(("groups", "ep"), None),
            P("tp", None),
            P("ep", None, "tp"),
            P("ep", None, "tp"),
            P("ep", "tp", None),
            P(("groups", "ep"), "tp", None),
            P(("groups", "ep"), "tp", None),
            P(("groups", "ep"), None, None),
            P(("groups", "ep"), None, None),
            P(("groups", "ep")),
        ),
        out_specs=(P(("groups", "ep"), "tp"), P(("groups", "ep"), "tp", None)),
        check_vma=False,
    )
```
